256 devices in a mesh: morton: 64 (over x, z, core), grp: 4 (over y).
Axes of the slice: x: 4, y: 4, z: 8, core: 2. Of those that a mesh axis runs over, the one named last changes fastest.
Arguments:
- multipoles: float32 [16384, 152], P(('morton', 'grp')), may hold values from -6 to 6
- chebyshev: float32 [16384, 560], P(('morton', 'grp')), may hold values from -6 to 6
- ghost_rows: int32 [4096, 64], P('morton'), may hold values from 0 to 255
- far_src: int32 [16384, 189], P(('morton', 'grp')), may hold values from 0 to 4351
- far_kind: int32 [16384, 189], P(('morton', 'grp')), may hold values from 0 to 15
- far_count: int32 [16384], P(('morton', 'grp')), may hold values from 1 to 189
- near_src: int32 [16384, 27], P(('morton', 'grp')), may hold values from 0 to 1087, as said below
- near_kind: int32 [16384, 27], P(('morton', 'grp')), may hold values from 0 to 3
- far_ops: float32 [16, 152, 152], replicated, may hold values from -0.046875 to 0.046875
- near_ops: float32 [4, 560, 560], replicated, may hold values from -0.046875 to 0.046875
- local_to_target: float32 [152, 560], replicated, may hold values from -0.5 to 0.5
Outputs:
- potential: float32 [16384, 560], P(('morton', 'grp'))
The draws below stay inside these ranges and needn't reach their ends.
Inputs may be any that keep to these rules, and one draw needn't show every extreme that they name: Entries below 256 name a box of the target's own range; the others name ghost number far_src - 256 of its far ghost list. Entries below 64 name a box of the target's own device; the others name ghost number near_src - 64 of its range's near ghost list.
All inputs are finite; a program needn't handle non-finite values.
Results may differ from the reference program's by a relative error of at most 0.0003.
Values sent between devices are 32-bit elements; how exact they have to be, the bound alone decides.
A program may use at most 64 MiB of HBM per device.

```python
import jax
import jax.numpy as jnp
from jax import lax

P_SIZE = 152
Q = 560
FAR = 189
NEAR = 27
FCLS = 16
NCLS = 4
CAP = 64
NCAP = 16
BOX_DEV = 64
RANGE = 256
BOXES = 16384
FTABLE = 4352
NTABLE = 1088
N_MORTON = 64
N_GRP = 4


def draw_near_src(key, part):
    pick_key = jax.random.fold_in(key, 11)
    own_key = jax.random.fold_in(key, 12)
    ghost_key = jax.random.fold_in(key, 13)
    shape = (BOXES, NEAR)
    selector = jax.random.randint(pick_key, shape, 0, 10)
    own_entry = jax.random.randint(own_key, shape, 0, BOX_DEV)
    ghost_entry = jax.random.randint(ghost_key, shape, BOX_DEV, NTABLE)
    return jnp.where(selector < 7, own_entry, ghost_entry).astype(jnp.int32)


def with_ends(values, stream_key, low, largest):
    dims = values.shape
    place = [jax.random.randint(jax.random.fold_in(stream_key, axis), (), 0, dims[axis]) for axis in range(len(dims))]
    values = values.at[tuple(place)].set(low)
    longest = dims.index(max(dims))
    place[longest] = (place[longest] + 1) % dims[longest]
    return values.at[tuple(place)].set(largest)


def shard_levels(key, shape, cuts, least, largest):
    def one(dim, shards_of):
        draws = jax.random.uniform(jax.random.fold_in(jax.random.fold_in(key, 6), dim), (shards_of,), jnp.float32, least / len(cuts), largest / len(cuts))
        return jnp.repeat(jnp.exp(draws), shape[dim] // shards_of).reshape((-1,) + (1,) * (len(shape) - dim - 1))

    level = one(*cuts[0])
    for cut in cuts[1:]:
        level = level * one(*cut)
    return level


def noise(key, extent, spread, most, shards=(), kind=jnp.bfloat16):
    values = spread * jax.random.normal(key, extent, jnp.float32)
    if shards:
        values = values * shard_levels(key, extent, shards, -0.22, 0.18)
    return jnp.clip(values, -most, most).astype(kind)


def setup_inputs(seed: int = 0) -> dict:
    keys = jax.random.split(jax.random.key(seed), 12)
    return {
        "multipoles": noise(keys[0], (BOXES, P_SIZE), 1.0, 6.0, ((0, 256),), jnp.float32),
        "chebyshev": noise(keys[1], (BOXES, Q), 1.0, 6.0, ((0, 256),), jnp.float32),
        "ghost_rows": with_ends(jax.random.randint(keys[2], (N_MORTON * N_MORTON, CAP), 0, RANGE), jax.random.fold_in(keys[2], 1), 0, RANGE - 1).astype(jnp.int32),
        "far_src": with_ends(jax.random.randint(keys[3], (BOXES, FAR), 0, FTABLE), jax.random.fold_in(keys[3], 1), 0, FTABLE - 1).astype(jnp.int32),
        "far_kind": with_ends(jax.random.randint(keys[4], (BOXES, FAR), 0, FCLS), jax.random.fold_in(keys[4], 1), 0, FCLS - 1).astype(jnp.int32),
        "far_count": with_ends(jax.random.randint(keys[5], (BOXES,), 1, FAR + 1), jax.random.fold_in(keys[5], 1), 1, FAR).astype(jnp.int32),
        "near_src": draw_near_src(jax.random.fold_in(keys[11], 71), 0),
        "near_kind": with_ends(jax.random.randint(keys[7], (BOXES, NEAR), 0, NCLS), jax.random.fold_in(keys[7], 1), 0, NCLS - 1).astype(jnp.int32),
        "far_ops": noise(keys[8], (FCLS, P_SIZE, P_SIZE), (P_SIZE * FAR // 2) ** -0.5, 0.046875, (), jnp.float32),
        "near_ops": noise(keys[9], (NCLS, Q, Q), (Q * NEAR) ** -0.5, 0.046875, (), jnp.float32),
        "local_to_target": noise(keys[10], (P_SIZE, Q), P_SIZE ** -0.5, 0.5, (), jnp.float32),
    }


def class_sum(lookup, indices, weight, class_ids, classes):
    targets, slot_count = indices.shape
    picked = lookup[indices] * weight[:, :, None]
    segment = (jnp.arange(targets, dtype=jnp.int32)[:, None] * classes + class_ids).reshape(-1)
    summed = jax.ops.segment_sum(picked.reshape(targets * slot_count, lookup.shape[1]), segment, num_segments=targets * classes)
    return summed.reshape(targets, classes, lookup.shape[1])


def evaluate(far_table, near_table, far_src, far_kind, far_count, near_src, near_kind, far_ops, near_ops, local_to_target):
    active = (jnp.arange(far_src.shape[1], dtype=jnp.int32)[None, :] < far_count[:, None]).astype(far_table.dtype)
    far_sum = class_sum(far_table, far_src, active, far_kind, far_ops.shape[0])
    local_field = jnp.einsum("tkp,kpq->tq", far_sum, far_ops, precision=lax.Precision.HIGHEST)
    unit_weight = jnp.ones(near_src.shape, near_table.dtype)
    near_sum = class_sum(near_table, near_src, unit_weight, near_kind, near_ops.shape[0])
    near_field = jnp.einsum("tkc,kcd->td", near_sum, near_ops, precision=lax.Precision.HIGHEST)
    return jnp.dot(local_field, local_to_target, precision=lax.Precision.HIGHEST) + near_field


def reference(multipoles, chebyshev, ghost_rows, far_src, far_kind, far_count, near_src, near_kind, far_ops, near_ops, local_to_target):
    starts = jnp.arange(N_MORTON, dtype=jnp.int32)[:, None] * RANGE
    ghost_table = ghost_rows.reshape(N_MORTON, N_MORTON, CAP)

    def device(position):
        anchor = (position // N_GRP).astype(jnp.int32)
        far_ids = (starts + ghost_table[:, anchor, :]).reshape(-1).astype(jnp.int32)
        near_ids = (starts + ghost_table[:, anchor, :NCAP]).reshape(-1).astype(jnp.int32)
        range_multi = lax.dynamic_slice_in_dim(multipoles, (anchor * RANGE).astype(jnp.int32), RANGE, 0)
        far_table = jnp.concatenate([range_multi, multipoles[far_ids]], axis=0)
        first = (position * BOX_DEV).astype(jnp.int32)
        own_cheb = lax.dynamic_slice_in_dim(chebyshev, first, BOX_DEV, 0)
        near_table = jnp.concatenate([own_cheb, chebyshev[near_ids]], axis=0)

        def mine(array):
            return lax.dynamic_slice_in_dim(array, first, BOX_DEV, 0)

        return evaluate(far_table, near_table, mine(far_src), mine(far_kind), mine(far_count), mine(near_src), mine(near_kind), far_ops, near_ops, local_to_target)

    result = lax.map(device, jnp.arange(N_MORTON * N_GRP, dtype=jnp.int32))
    return result.reshape(BOXES, Q)
```

```python
import functools

import jax
import jax.numpy as jnp
from jax import lax
from jax.experimental import pallas as pl
from jax.experimental.pallas import tpu as pltpu
from jax.sharding import PartitionSpec as P

MESH = pl.DeviceIdType.MESH
BF = jnp.bfloat16
F32 = jnp.float32
I32 = jnp.int32

PW = 152
TW = PW - 128
QW = 560
QP = 640
FAR = 189
NEAR = 27
NEAR_AT = 192
CAP = 64
NCAP = 16
FCLS = 16
NCLS = 4
BOX = 64
KEYS = 160
SW = 1152


def split2(x):
    hi = x.astype(BF)
    return hi, (x - hi.astype(F32)).astype(BF)


def dot(a, b):
    return jnp.dot(a, b, preferred_element_type=F32)


def iota(shape, dim):
    return lax.broadcasted_iota(I32, shape, dim)


def evaluate(
    sizes,
    multi,
    cheb,
    ghost,
    idx,
    far_ops,
    near_ops,
    to_target,
    out,
    mall,
    call,
    iall,
    send_f,
    send_n,
    recv_f,
    recv_n,
    pick_f,
    pick_n,
    pick_e,
    w_pick,
    key_l,
    key_r,
    count,
    ncount,
    w_main,
    w_tail,
    w_near,
    far_main,
    far_tail,
    ops_f,
    ops_n,
    ops_t,
    f_hi,
    f_lo,
    n_hi,
    n_lo,
    t_hi,
    t_lo,
    local_sum,
    near_sum,
    nh,
    nl,
    rs_send,
    rs_recv,
    y_send,
    y_recv,
    f_send,
    f_recv,
    n_send,
    n_recv,
    r_send,
    r_recv,
    load,
):
    xs, zs, cs = sizes
    ranges = xs * zs * cs
    me = lax.axis_index("morton")
    h = lax.axis_index("grp")
    my_x = me // (zs * cs)
    my_z = (me // cs) % zs
    my_c = me % cs

    def helper(d):
        return (me, (h + d) % 4)

    def peer(o):
        zz = o % zs
        dz = ((zz + 1) // 2) * (1 - 2 * ((zz + 1) % 2))
        dx = (o // zs) % xs
        dc = o // (zs * xs)
        x = (my_x + dx) % xs
        z = (my_z + dz + zs) % zs
        return (x * zs + z) * cs + (my_c + dc) % cs

    loads = [
        pltpu.make_async_copy(far_ops, ops_f, load.at[0]),
        pltpu.make_async_copy(near_ops, ops_n, load.at[1]),
        pltpu.make_async_copy(to_target, ops_t, load.at[2]),
    ]
    for copy in loads:
        copy.start()

    barrier = pltpu.get_barrier_semaphore()
    for d in range(1, 4):
        pl.semaphore_signal(barrier, inc=1, device_id=helper(d), device_id_type=MESH)

    def greet(o, _):
        pl.semaphore_signal(barrier, inc=1, device_id=(peer(o), h), device_id_type=MESH)
        return 0

    lax.fori_loop(1, ranges, greet, 0)
    pl.semaphore_wait(barrier, ranges - 1 + 3)

    def to_helpers(k, src, dst):
        copies = []
        for d in range(1, 4):
            copies.append(
                pltpu.make_async_remote_copy(
                    src_ref=src,
                    dst_ref=dst.at[h],
                    send_sem=y_send.at[3 * k + d - 1],
                    recv_sem=y_recv.at[3 * k + d - 1],
                    device_id=helper(d),
                    device_id_type=MESH,
                )
            )
        return copies

    y_copies = [to_helpers(0, multi, mall), to_helpers(1, cheb, call), to_helpers(2, idx, iall)]
    for group in y_copies:
        for copy in group:
            copy.start()
    mall[h] = multi[...]
    call[h] = cheb[...]
    iall[h] = idx[...]

    rows = ranges * 8
    step = min(128, rows)
    ghost_b = ghost[...].astype(F32).astype(BF)
    lane64 = iota((step, CAP), 1)
    sub64 = iota((step, CAP), 0) % 8
    lane256 = iota((step, 256), 1)
    low_half = (iota((step, 256), 0) % 8) < 4

    def build_pick(i, _):
        at = pl.multiple_of(i * step, step)
        own = ((iota((step, ranges), 0) + at) // 8) == iota((step, ranges), 1)
        each = dot(jnp.where(own, 1.0, 0.0).astype(BF), ghost_b)

        def chosen(slot):
            one = jnp.sum(jnp.where(lane64 == slot, each, 0.0), axis=1, keepdims=True)
            return lane256 == one.astype(I32)

        def put(ref, col, mask):
            ref[pl.ds(at, step), col : col + 256] = jnp.where(mask, 1.0, 0.0).astype(BF)

        put(pick_f, 0, chosen(16 * h + sub64))
        put(pick_f, 256, chosen(16 * h + 8 + sub64))
        near = chosen(4 * h + sub64 % 4)
        put(pick_n, 0, near & low_half)
        put(pick_n, 256, near & jnp.logical_not(low_half))
        for t in range(4):
            put(pick_e, 256 * t, chosen(16 * h + 4 * t + sub64 % 4) & low_half)
        return 0

    lax.fori_loop(0, rows // step, build_pick, 0)

    for copy in y_copies[0]:
        copy.wait()

    range_multi = mall[...].reshape(256, PW)
    hi, lo = split2(range_multi[:, :128])
    w_pick[0:256, 0:128] = hi
    w_pick[0:256, 128:256] = lo
    messages = step // 8

    def pick_far(i, _):
        at = pl.multiple_of(i * step, step)
        to = pl.ds(i * messages, messages)
        for half in range(2):
            both = dot(pick_f[pl.ds(at, step), 256 * half : 256 * half + 256], w_pick[0:256, :])
            send_f[to, 8 * half : 8 * half + 8, :] = (both[:, :128] + both[:, 128:]).reshape(
                messages, 8, 128
            )
        return 0

    lax.fori_loop(0, rows // step, pick_far, 0)

    def block(s, n):
        return pl.ds(pl.multiple_of(s * n, n), n)

    def exchange(src, dst, s_sem, r_sem, o):
        to = peer(o)
        return pltpu.make_async_remote_copy(
            src_ref=src.at[to],
            dst_ref=dst.at[block(me, src.shape[1]), :],
            send_sem=s_sem.at[o],
            recv_sem=r_sem.at[o],
            device_id=(to, h),
            device_id_type=MESH,
        )

    def send_far(o, _):
        exchange(send_f, recv_f, f_send, f_recv, o).start()
        return 0

    lax.fori_loop(1, ranges, send_far, 0)
    recv_f[block(me, 16), :] = send_f[me]

    tail = jnp.concatenate([range_multi[:, 128:], jnp.zeros((256, 128 - TW), F32)], axis=1)
    hi, lo = split2(tail)
    for t in range(4):
        moved = pltpu.roll(tail, TW * t, axis=1) if t else tail
        hi, lo = split2(moved)
        w_pick[256 * (t + 1) : 256 * (t + 2), 0:128] = hi
        w_pick[256 * (t + 1) : 256 * (t + 2), 128:256] = lo

    for copy in y_copies[1]:
        copy.wait()

    range_cheb = call[...].reshape(256, QW)
    for l in range(5):
        if l < 4:
            part = range_cheb[:, 128 * l : 128 * l + 128]
        else:
            part = jnp.concatenate(
                [range_cheb[:, 512:], jnp.zeros((256, QP - QW), F32)], axis=1
            )
        hi, lo = split2(part)
        w_pick[256 * (l + 5) : 256 * (l + 6), 0:128] = hi
        w_pick[256 * (l + 5) : 256 * (l + 6), 128:256] = lo

    def pick_near(i, _):
        at = pl.multiple_of(i * step, step)
        to = pl.ds(i * messages, messages)
        near = pick_n[pl.ds(at, step), :]
        for half in range(2):
            both = dot(near, w_pick[256 * (5 + 2 * half) : 256 * (7 + 2 * half), :])
            send_n[to, 8 * half : 8 * half + 8, :] = (both[:, :128] + both[:, 128:]).reshape(
                messages, 8, 128
            )
        both = dot(pick_e[pl.ds(at, step), 0:1024], w_pick[256:1280, :])
        both = both + dot(near[:, 256:], w_pick[256 * 9 : 256 * 10, :])
        send_n[to, 16:24, :] = (both[:, :128] + both[:, 128:]).reshape(messages, 8, 128)
        return 0

    lax.fori_loop(0, rows // step, pick_near, 0)

    def send_near(o, _):
        exchange(send_n, recv_n, n_send, n_recv, o).start()
        return 0

    lax.fori_loop(1, ranges, send_near, 0)
    recv_n[block(me, 24), :] = send_n[me]

    for copy in loads:
        copy.wait()
    f_hi[...] = jnp.zeros_like(f_hi)
    f_lo[...] = jnp.zeros_like(f_lo)
    n_hi[...] = jnp.zeros_like(n_hi)
    n_lo[...] = jnp.zeros_like(n_lo)
    t_hi[...] = jnp.zeros_like(t_hi)
    t_lo[...] = jnp.zeros_like(t_lo)

    def split_far_op(k, _):
        hi, lo = split2(ops_f[k])
        f_hi[k, 0:PW, 0:PW] = hi
        f_lo[k, 0:PW, 0:PW] = lo
        return 0

    lax.fori_loop(0, FCLS, split_far_op, 0)

    def split_near_op(k, _):
        hi, lo = split2(ops_n[k])
        n_hi[k, 0:QW, 0:QW] = hi
        n_lo[k, 0:QW, 0:QW] = lo
        return 0

    lax.fori_loop(0, NCLS, split_near_op, 0)
    hi, lo = split2(ops_t[...])
    t_hi[0:PW, 0:QW] = hi
    t_lo[0:PW, 0:QW] = lo

    for copy in y_copies[2]:
        copy.wait()

    lane = iota((BOX, 256), 1)

    def keys(g, _):
        src = iall[g, :, 0:256]
        kind = iall[g, :, 256:512]
        live = kind[:, 255:256]
        is_far = lane < live
        is_near = (lane >= NEAR_AT) & (lane < NEAR_AT + NEAR)
        slot = src - 256
        s = slot >> 6
        c = slot & 63
        own = src < 256
        far_on = jnp.where(own, src >> 6, c >> 4) == h
        c = c & 15
        far_l = jnp.where(own, 128, (c >> 1) * 16) + kind
        far_r = jnp.where(own, src & 63, (c & 1) * 64 + s)
        slot = src - BOX
        s = slot >> 4
        c = slot & 15
        own = src < BOX
        near_on = jnp.where(own, g, c >> 2) == h
        c = c & 3
        near_l = jnp.where(own, 152, 144 + (c >> 1) * 4) + kind
        near_r = jnp.where(own, src, (c & 1) * 64 + s)
        on = (is_near & near_on) | (is_far & far_on)
        left = jnp.where(is_near, near_l, far_l)
        right = jnp.where(is_near, near_r, far_r)
        at = pl.ds(pl.multiple_of(g * BOX, BOX), BOX)
        key_l[at, :] = jnp.where(on, left, -1).astype(F32)
        key_r[at, :] = right.astype(F32)
        return 0

    lax.fori_loop(0, 4, keys, 0)

    sub16 = iota((16, 256), 0).astype(F32).astype(BF)
    unroll = 2

    def count_box(i, _):
        for u in range(unroll):
            b = i * unroll + u
            kl = jnp.broadcast_to(key_l[pl.ds(b, 1), :], (16, 256)).astype(BF)
            kr = jnp.broadcast_to(key_r[pl.ds(b, 1), :], (16, 256)).astype(BF)
            one = jnp.ones((16, 256), BF)
            zero = jnp.zeros((16, 256), BF)
            left = jnp.concatenate(
                [
                    jnp.where(kl == sub16 + jnp.asarray(16 * r, BF), one, zero)
                    for r in range(KEYS // 16)
                ],
                axis=0,
            )
            right = jnp.concatenate(
                [jnp.where(kr == sub16 + jnp.asarray(16 * r, BF), one, zero) for r in range(8)],
                axis=0,
            )
            both = lax.dot_general(
                left, right, (((1,), (1,)), ((), ())), preferred_element_type=F32
            )
            at = pl.ds(pl.multiple_of(b * 16, 16), 16)
            for r in range(9):
                count[at, 128 * r : 128 * r + 128] = both[16 * r : 16 * r + 16, :].astype(BF)
            ncount[at, :] = both[144:160, :]
        return 0

    lax.fori_loop(0, 4 * BOX // unroll, count_box, 0)

    own_cheb = jnp.concatenate([cheb[...], jnp.zeros((BOX, QP - QW), F32)], axis=1)
    own_cheb = jnp.concatenate([own_cheb, jnp.zeros((BOX, QP), F32)], axis=0)
    own_hi, own_lo = split2(own_cheb)

    def near_own(k, _):
        m = ncount[pl.ds(8 + k, 256, stride=16), :].astype(BF)
        near_sum[k] = dot(m, own_hi) + dot(m, own_lo)
        return 0

    lax.fori_loop(0, NCLS, near_own, 0)

    w_main[...] = jnp.zeros_like(w_main)
    w_tail[...] = jnp.zeros_like(w_tail)
    hi, lo = split2(multi[:, 0:128])
    w_main[1024:1088, 0:128] = hi
    w_main[1024:1088, 128:256] = lo

    def put_tail(at, x):
        high = x.astype(BF).astype(F32)
        keep = iota(x.shape, 1) < TW
        packed = jnp.where(keep, high, 0.0) + pltpu.roll(jnp.where(keep, x - high, 0.0), TW, axis=1)
        w_tail[at, :] = packed.astype(BF)

    put_tail(
        pl.ds(1024, BOX),
        jnp.concatenate([multi[:, 128:PW], jnp.zeros((BOX, 128 - TW), F32)], axis=1),
    )

    def far_arrived(o, _):
        exchange(send_f, recv_f, f_send, f_recv, o).wait()
        return 0

    lax.fori_loop(1, ranges, far_arrived, 0)
    for c in range(16):
        hi, lo = split2(recv_f[pl.ds(c, ranges, stride=16), :])
        w_main[64 * c : 64 * c + ranges, 0:128] = hi
        w_main[64 * c : 64 * c + ranges, 128:256] = lo

    def far_rows(i, _):
        at = pl.ds(pl.multiple_of(i * 256, 256), 256)
        both = dot(count[at, :], w_main[...])
        far_main[at, :] = both[:, :128] + both[:, 128:]
        return 0

    lax.fori_loop(0, 16, far_rows, 0)

    def near_arrived(o, _):
        exchange(send_n, recv_n, n_send, n_recv, o).wait()
        return 0

    lax.fori_loop(1, ranges, near_arrived, 0)
    for q in range(4):
        x = recv_n[pl.ds(16 + q, ranges, stride=24), :]
        for t in range(4):
            moved = pltpu.roll(x, 128 - TW * t, axis=1) if t else x
            at = 256 * t + 64 * q
            put_tail(pl.ds(at, ranges), moved)
    if ranges < 64:
        w_near[...] = jnp.zeros_like(w_near)
    for c in range(4):
        for l in range(5):
            row = 4 * l + c if l < 4 else 20 + c
            x = recv_n[pl.ds(row, ranges, stride=24), :]
            hi, lo = split2(x)
            w_near[64 * c : 64 * c + ranges, 128 * l : 128 * l + 128] = hi
            w_near[64 * c : 64 * c + ranges, QP + 128 * l : QP + 128 * l + 128] = lo

    def far_rows_tail(i, _):
        at = pl.ds(pl.multiple_of(i * 256, 256), 256)
        both = dot(count[at, :], w_tail[...])
        far_tail[at, :] = both + pltpu.roll(both, 128 - TW, axis=1)
        return 0

    lax.fori_loop(0, 16, far_rows_tail, 0)

    local_sum[...] = jnp.zeros_like(local_sum)

    def far_class(k, _):
        at = pl.ds(k, 256, stride=16)
        hi, lo = split2(jnp.concatenate([far_main[at, :], far_tail[at, :]], axis=1))
        local_sum[...] += dot(hi, f_hi[k]) + dot(hi, f_lo[k]) + dot(lo, f_hi[k])
        return 0

    lax.fori_loop(0, FCLS, far_class, 0)

    def near_class(k, _):
        m = jnp.concatenate(
            [ncount[pl.ds(k, 256, stride=16), :], ncount[pl.ds(4 + k, 256, stride=16), :]], axis=1
        ).astype(BF)
        total = near_sum[k] + dot(m, w_near[:, 0:QP]) + dot(m, w_near[:, QP:])
        hi, lo = split2(total)
        nh[k] = hi
        nl[k] = lo
        return 0

    lax.fori_loop(0, NCLS, near_class, 0)

    lh, ll = split2(local_sum[...])
    back = []
    for n, (n0, w) in enumerate(((0, 256), (256, 256), (512, 128))):
        cols = slice(n0, n0 + w)
        total = dot(lh, t_hi[:, cols]) + dot(lh, t_lo[:, cols]) + dot(ll, t_hi[:, cols])
        for k in range(NCLS):
            total = total + (
                dot(nh[k], n_hi[k, :, cols])
                + dot(nh[k], n_lo[k, :, cols])
                + dot(nl[k], n_hi[k, :, cols])
            )
        rs_send[:, :, cols] = total.reshape(4, BOX, w)
        for d in (2, 1, 3):
            copy = pltpu.make_async_remote_copy(
                src_ref=rs_send.at[(h + d) % 4, :, cols],
                dst_ref=rs_recv.at[d - 1, :, cols],
                send_sem=r_send.at[3 * n + d - 1],
                recv_sem=r_recv.at[3 * n + d - 1],
                device_id=helper(d),
                device_id_type=MESH,
            )
            copy.start()
            back.append(copy)
    for copy in back:
        copy.wait()
    total = rs_send[h] + rs_recv[0] + rs_recv[1] + rs_recv[2]
    out[...] = total[:, :QW]


def shards(sizes, multi, cheb, ghost, far_src, far_kind, far_count, near_src, near_kind, far_ops, near_ops, to_target):
    ranges = sizes[0] * sizes[1] * sizes[2]

    def lanes(far, near, last):
        gap = jnp.zeros((BOX, NEAR_AT - FAR), I32)
        rest = jnp.zeros((BOX, 255 - NEAR_AT - NEAR), I32)
        return jnp.concatenate([far, gap, near, rest, last], axis=1)

    idx = jnp.concatenate(
        [
            lanes(far_src, near_src, jnp.zeros((BOX, 1), I32)),
            lanes(far_kind, near_kind, far_count[:, None]),
        ],
        axis=1,
    )
    rows = ranges * 8
    vmem = pl.BlockSpec(memory_space=pltpu.VMEM)
    hbm = pl.BlockSpec(memory_space=pl.ANY)
    dma = pltpu.SemaphoreType.DMA
    return pl.pallas_call(
        functools.partial(evaluate, sizes),
        out_shape=jax.ShapeDtypeStruct((BOX, QW), F32),
        in_specs=[vmem] * 4 + [hbm] * 3,
        out_specs=vmem,
        scratch_shapes=[
            pltpu.VMEM((4, BOX, PW), F32),
            pltpu.VMEM((4, BOX, QW), F32),
            pltpu.VMEM((4, BOX, 512), I32),
            pltpu.VMEM((ranges, 16, 128), F32),
            pltpu.VMEM((ranges, 24, 128), F32),
            pltpu.VMEM((ranges * 16, 128), F32),
            pltpu.VMEM((ranges * 24, 128), F32),
            pltpu.VMEM((rows, 512), BF),
            pltpu.VMEM((rows, 512), BF),
            pltpu.VMEM((rows, 1024), BF),
            pltpu.VMEM((2560, 256), BF),
            pltpu.VMEM((256, 256), F32),
            pltpu.VMEM((256, 256), F32),
            pltpu.VMEM((4096, SW), BF),
            pltpu.VMEM((4096, 128), F32),
            pltpu.VMEM((SW, 256), BF),
            pltpu.VMEM((SW, 128), BF),
            pltpu.VMEM((256, 2 * QP), BF),
            pltpu.VMEM((4096, 128), F32),
            pltpu.VMEM((4096, 128), F32),
            pltpu.VMEM((FCLS, PW, PW), F32),
            pltpu.VMEM((NCLS, QW, QW), F32),
            pltpu.VMEM((PW, QW), F32),
            pltpu.VMEM((FCLS, 256, 256), BF),
            pltpu.VMEM((FCLS, 256, 256), BF),
            pltpu.VMEM((NCLS, QP, QP), BF),
            pltpu.VMEM((NCLS, QP, QP), BF),
            pltpu.VMEM((256, QP), BF),
            pltpu.VMEM((256, QP), BF),
            pltpu.VMEM((256, 256), F32),
            pltpu.VMEM((NCLS, 256, QP), F32),
            pltpu.VMEM((NCLS, 256, QP), BF),
            pltpu.VMEM((NCLS, 256, QP), BF),
            pltpu.VMEM((4, BOX, QP), F32),
            pltpu.VMEM((3, BOX, QP), F32),
            dma((9,)),
            dma((9,)),
            dma((ranges,)),
            dma((ranges,)),
            dma((ranges,)),
            dma((ranges,)),
            dma((9,)),
            dma((9,)),
            dma((3,)),
        ],
        compiler_params=pltpu.CompilerParams(
            collective_id=0, has_side_effects=True, vmem_limit_bytes=60 * 1024 * 1024
        ),
        name="evaluate",
    )(multi, cheb, ghost, idx, far_ops, near_ops, to_target)


def solution(mesh, sizes=(4, 8, 2)):
    rows = P(("morton", "grp"), None)
    placed = (
        rows,
        rows,
        P("morton", None),
        rows,
        rows,
        P(("morton", "grp")),
        rows,
        rows,
        P(),
        P(),
        P(),
    )
    return jax.shard_map(
        functools.partial(shards, sizes), mesh=mesh, in_specs=placed, out_specs=rows, check_vma=False
    )
```

```python
import functools

import jax
import jax.numpy as jnp
from jax import lax
from jax.experimental import pallas as pl
from jax.experimental.pallas import tpu as pltpu
from jax.sharding import PartitionSpec as P

MESH = pl.DeviceIdType.MESH
BF = jnp.bfloat16
F32 = jnp.float32
I32 = jnp.int32

PW = 152
TW = PW - 128
QW = 560
QP = 640
FAR = 189
NEAR = 27
NEAR_AT = 192
CAP = 64
NCAP = 16
FCLS = 16
NCLS = 4
BOX = 64
KEYS = 160
SW = 1152


def split2(x):
    hi = x.astype(BF)
    return hi, (x - hi.astype(F32)).astype(BF)


def dot(a, b):
    return jnp.dot(a, b, preferred_element_type=F32)


def iota(shape, dim):
    return lax.broadcasted_iota(I32, shape, dim)


def evaluate(
    sizes,
    multi,
    cheb,
    ghost,
    far_src,
    far_kind,
    far_count,
    near_src,
    near_kind,
    far_ops,
    near_ops,
    to_target,
    out,
    mall,
    call,
    iall,
    send_f,
    send_n,
    recv_f,
    recv_n,
    pick_f,
    pick_n,
    pick_e,
    w_pick,
    turned,
    key_l,
    key_r,
    count,
    ncount,
    w_main,
    w_tail,
    w_near,
    far_main,
    far_tail,
    ops_f,
    ops_n,
    ops_t,
    f_hi,
    f_lo,
    n_hi,
    n_lo,
    t_hi,
    t_lo,
    local_sum,
    near_sum,
    parts,
    rs_send,
    rs_recv,
    y_send,
    y_recv,
    f_send,
    f_recv,
    n_send,
    n_recv,
    r_send,
    r_recv,
    load,
):
    xs, zs, cs = sizes
    ranges = xs * zs * cs
    me = lax.axis_index("morton")
    h = lax.axis_index("grp")
    my_x = lax.div(me, zs * cs)
    my_z = lax.rem(lax.div(me, cs), zs)
    my_c = lax.rem(me, cs)

    def helper(d):
        return (me, lax.rem(h + d, 4))

    def peer(o):
        zz = lax.rem(o, zs)
        up = lax.div(zz + 1, 2)
        dz = up + lax.rem(zz + 1, 2) * (zs - 2 * up)
        dx = lax.rem(lax.div(o, zs), xs)
        dc = lax.div(o, zs * xs)
        x = lax.rem(my_x + dx, xs)
        z = lax.rem(my_z + dz, zs)
        return (x * zs + z) * cs + lax.rem(my_c + dc, cs)

    loads = [
        pltpu.make_async_copy(far_ops, ops_f, load.at[0]),
        pltpu.make_async_copy(near_ops, ops_n, load.at[1]),
        pltpu.make_async_copy(to_target, ops_t, load.at[2]),
    ]
    for copy in loads:
        copy.start()

    lane64 = iota((BOX, 128), 1)
    tail = jnp.concatenate([multi[:, 128:], jnp.zeros((BOX, 128 - TW), F32)], axis=1)
    rest = jnp.concatenate([cheb[:, 512:], jnp.zeros((BOX, QP - QW), F32)], axis=1)
    mall[h] = multi[:, 0:128]
    call[h, :, 0:512] = cheb[:, 0:512]
    call[h, :, 512:QP] = rest + pltpu.roll(tail, QW - 512, axis=1)
    turned[...] = jnp.zeros_like(turned)
    turned[0:NEAR, 0:BOX] = near_src[...].astype(F32)
    turned[32 : 32 + NEAR, 0:BOX] = near_kind[...].astype(F32)
    turned[64:65, 0:BOX] = far_count[...].astype(F32)
    near = turned[...].T[0:BOX, :]
    at_near = (lane64 >= 64) & (lane64 < 64 + NEAR)

    def second(far, shift):
        far = jnp.concatenate([far[:, 128:], jnp.zeros((BOX, 256 - FAR), I32)], axis=1)
        moved = pltpu.roll(near, shift, axis=1).astype(I32)
        return jnp.where(at_near, moved, jnp.where(lane64 < FAR - 128, far, 0))

    iall[h, :, 0:128] = far_src[:, 0:128]
    iall[h, :, 128:256] = second(far_src, 64)
    iall[h, :, 256:384] = far_kind[:, 0:128]
    live = pltpu.roll(near, 63, axis=1).astype(I32)
    iall[h, :, 384:512] = jnp.where(lane64 == 127, live, second(far_kind, 32))

    barrier = pltpu.get_barrier_semaphore()
    for d in range(1, 4):
        pl.semaphore_signal(barrier, inc=1, device_id=helper(d), device_id_type=MESH)

    def greet(o, _):
        pl.semaphore_signal(barrier, inc=1, device_id=(peer(o), h), device_id_type=MESH)
        return 0

    lax.fori_loop(1, ranges, greet, 0)

    rows = ranges * 8
    step = min(128, rows)
    ghost_b = ghost[...].astype(F32).astype(BF)
    lane_c = iota((step, CAP), 1)
    sub = iota((step, CAP), 0) % 8
    lane256 = iota((step, 256), 1)
    low_half = (iota((step, 256), 0) % 8) < 4

    def build_pick(i, _):
        at = pl.multiple_of(i * step, step)
        own = ((iota((step, ranges), 0) + at) // 8) == iota((step, ranges), 1)
        each = dot(jnp.where(own, 1.0, 0.0).astype(BF), ghost_b)

        def chosen(slot):
            one = jnp.sum(jnp.where(lane_c == slot, each, 0.0), axis=1, keepdims=True)
            return lane256 == one.astype(I32)

        def put(ref, col, mask):
            ref[pl.ds(at, step), col : col + 256] = jnp.where(mask, 1.0, 0.0).astype(BF)

        put(pick_f, 0, chosen(16 * h + sub))
        put(pick_f, 256, chosen(16 * h + 8 + sub))
        near = chosen(4 * h + sub % 4)
        put(pick_n, 0, near & low_half)
        put(pick_n, 256, near & jnp.logical_not(low_half))
        for t in range(4):
            put(pick_e, 256 * t, chosen(16 * h + 4 * t + sub % 4) & low_half)
        return 0

    lax.fori_loop(0, rows // step, build_pick, 0)

    for copy in loads:
        copy.wait()
    for ref in (f_hi, f_lo, n_hi, n_lo, t_hi, t_lo, near_sum, w_main, w_tail):
        ref[...] = jnp.zeros_like(ref)

    def split_far_op(k, _):
        hi, lo = split2(ops_f[k])
        at = pl.ds(pl.multiple_of(k * 256, 256), PW)
        f_hi[at, 0:PW] = hi
        f_lo[at, 0:PW] = lo
        return 0

    lax.fori_loop(0, FCLS, split_far_op, 0)

    def split_near_op(k, _):
        hi, lo = split2(ops_n[k])
        at = pl.ds(pl.multiple_of(k * QP, QP), QW)
        n_hi[at, 0:QW] = hi
        n_lo[at, 0:QW] = lo
        return 0

    lax.fori_loop(0, NCLS, split_near_op, 0)
    hi, lo = split2(ops_t[...])
    t_hi[0:PW, 0:QW] = hi
    t_lo[0:PW, 0:QW] = lo

    pl.semaphore_wait(barrier, ranges - 1 + 3)

    def to_helpers(k, ref):
        copies = []
        for d in (2, 1, 3):
            copies.append(
                pltpu.make_async_remote_copy(
                    src_ref=ref.at[h],
                    dst_ref=ref.at[h],
                    send_sem=y_send.at[3 * k + d - 1],
                    recv_sem=y_recv.at[3 * k + d - 1],
                    device_id=helper(d),
                    device_id_type=MESH,
                )
            )
        return copies

    y_copies = [to_helpers(0, mall), to_helpers(1, call), to_helpers(2, iall)]
    for group in y_copies:
        for copy in group:
            copy.start()

    lane = iota((BOX, 256), 1)

    def keys(g):
        src = iall[g, :, 0:256]
        kind = iall[g, :, 256:512]
        live = kind[:, 255:256]
        is_far = (lane < live) & (lane < FAR)
        is_near = (lane >= NEAR_AT) & (lane < NEAR_AT + NEAR)
        slot = src - 256
        s = slot >> 6
        c = slot & 63
        own = src < 256
        far_on = jnp.where(own, src >> 6, c >> 4) == h
        c = c & 15
        far_l = jnp.where(own, 128, (c >> 1) * 16) + kind
        far_r = jnp.where(own, src & 63, (c & 1) * 64 + s)
        slot = src - BOX
        s = slot >> 4
        c = slot & 15
        own = src < BOX
        near_on = jnp.where(own, g, c >> 2) == h
        c = c & 3
        near_l = jnp.where(own, 152, 144 + (c >> 1) * 4) + kind
        near_r = jnp.where(own, src, (c & 1) * 64 + s)
        on = (is_near & near_on) | (is_far & far_on)
        left = jnp.where(is_near, near_l, far_l)
        right = jnp.where(is_near, near_r, far_r)
        at = pl.ds(pl.multiple_of(g * BOX, BOX), BOX)
        key_l[at, :] = jnp.where(on, left, -1).astype(F32)
        key_r[at, :] = right.astype(F32)

    sub16 = iota((16, 256), 0).astype(F32).astype(BF)
    unroll = 8

    def count_box(b):
        kl = jnp.broadcast_to(key_l[pl.ds(b, 1), :], (16, 256)).astype(BF)
        kr = jnp.broadcast_to(key_r[pl.ds(b, 1), :], (16, 256)).astype(BF)
        one = jnp.ones((16, 256), BF)
        zero = jnp.zeros((16, 256), BF)
        left = jnp.concatenate(
            [
                jnp.where(kl == sub16 + jnp.asarray(16 * r, BF), one, zero)
                for r in range(KEYS // 16)
            ],
            axis=0,
        )
        right = jnp.concatenate(
            [jnp.where(kr == sub16 + jnp.asarray(16 * r, BF), one, zero) for r in range(8)],
            axis=0,
        )
        return lax.dot_general(
            left, right, (((1,), (1,)), ((), ())), preferred_element_type=F32
        )

    def count_block(g):
        def some(i, _):
            first = g * BOX + i * unroll
            found = [count_box(first + u) for u in range(unroll)]
            for u, both in enumerate(found):
                at = pl.ds(pl.multiple_of((first + u) * 16, 16), 16)
                for r in range(9):
                    count[at, 128 * r : 128 * r + 128] = both[16 * r : 16 * r + 16, :].astype(BF)
                ncount[at, :] = both[144:160, :]
            return 0

        lax.fori_loop(0, BOX // unroll, some, 0)

    keys(h)
    count_block(h)

    for copy in y_copies[0]:
        copy.wait()

    hi, lo = split2(mall[...].reshape(256, 128))
    w_pick[0:256, 0:128] = hi
    w_pick[0:256, 128:256] = lo
    messages = step // 8

    def pick_far(i, _):
        at = pl.multiple_of(i * step, step)
        to = pl.ds(i * messages, messages)
        for half in range(2):
            both = dot(pick_f[pl.ds(at, step), 256 * half : 256 * half + 256], w_pick[0:256, :])
            send_f[to, 8 * half : 8 * half + 8, :] = (both[:, :128] + both[:, 128:]).reshape(
                messages, 8, 128
            )
        return 0

    lax.fori_loop(0, rows // step, pick_far, 0)

    def block(s, n):
        return pl.ds(pl.multiple_of(s * n, n), n)

    def exchange(src, dst, s_sem, r_sem, o):
        to = peer(o)
        return pltpu.make_async_remote_copy(
            src_ref=src.at[to],
            dst_ref=dst.at[block(me, src.shape[1]), :],
            send_sem=s_sem.at[o],
            recv_sem=r_sem.at[o],
            device_id=(to, h),
            device_id_type=MESH,
        )

    def send_far(o, _):
        exchange(send_f, recv_f, f_send, f_recv, o).start()
        return 0

    lax.fori_loop(1, ranges, send_far, 0)
    recv_f[block(me, 16), :] = send_f[me]

    own_cheb = jnp.concatenate([cheb[:, 0:512], rest], axis=1)
    own_cheb = jnp.concatenate([own_cheb, jnp.zeros((BOX, QP), F32)], axis=0)
    own_hi, own_lo = split2(own_cheb)
    mine = pl.ds(pl.multiple_of(h * BOX, BOX), BOX)
    for k in range(NCLS):
        m = ncount[pl.ds(h * 16 * BOX + 8 + k, BOX, stride=16), :].astype(BF)
        near_sum[k, mine, :] = dot(m, own_hi) + dot(m, own_lo)

    hi, lo = split2(multi[:, 0:128])
    w_main[1024:1088, 0:128] = hi
    w_main[1024:1088, 128:256] = lo

    def put_tail(at, x):
        high = x.astype(BF).astype(F32)
        keep = iota(x.shape, 1) < TW
        packed = jnp.where(keep, high, 0.0) + pltpu.roll(jnp.where(keep, x - high, 0.0), TW, axis=1)
        w_tail[at, :] = packed.astype(BF)

    put_tail(pl.ds(1024, BOX), tail)

    for copy in y_copies[1]:
        copy.wait()

    lane_t = iota((256, 128), 1)
    last = call[:, :, 512:QP].reshape(256, 128)
    tails = jnp.where(lane_t < TW, pltpu.roll(last, 128 - (QW - 512), axis=1), 0.0)
    for t in range(4):
        hi, lo = split2(pltpu.roll(tails, TW * t, axis=1) if t else tails)
        w_pick[256 * (t + 1) : 256 * (t + 2), 0:128] = hi
        w_pick[256 * (t + 1) : 256 * (t + 2), 128:256] = lo
    for l in range(5):
        if l < 4:
            part = call[:, :, 128 * l : 128 * l + 128].reshape(256, 128)
        else:
            part = jnp.where(lane_t < QW - 512, last, 0.0)
        hi, lo = split2(part)
        w_pick[256 * (l + 5) : 256 * (l + 6), 0:128] = hi
        w_pick[256 * (l + 5) : 256 * (l + 6), 128:256] = lo

    def pick_near(i, _):
        at = pl.multiple_of(i * step, step)
        to = pl.ds(i * messages, messages)
        near = pick_n[pl.ds(at, step), :]
        for half in range(2):
            both = dot(near, w_pick[256 * (5 + 2 * half) : 256 * (7 + 2 * half), :])
            send_n[to, 8 * half : 8 * half + 8, :] = (both[:, :128] + both[:, 128:]).reshape(
                messages, 8, 128
            )
        both = dot(pick_e[pl.ds(at, step), 0:1024], w_pick[256:1280, :])
        both = both + dot(near[:, 256:], w_pick[256 * 9 : 256 * 10, :])
        send_n[to, 16:24, :] = (both[:, :128] + both[:, 128:]).reshape(messages, 8, 128)
        return 0

    lax.fori_loop(0, rows // step, pick_near, 0)

    def send_near(o, _):
        exchange(send_n, recv_n, n_send, n_recv, o).start()
        return 0

    lax.fori_loop(1, ranges, send_near, 0)
    recv_n[block(me, 24), :] = send_n[me]

    for copy in y_copies[2]:
        copy.wait()

    def other_block(d, _):
        g = lax.rem(h + d, 4)
        keys(g)
        count_block(g)
        return 0

    lax.fori_loop(1, 4, other_block, 0)

    def far_arrived(o, _):
        exchange(send_f, recv_f, f_send, f_recv, o).wait()
        return 0

    lax.fori_loop(1, ranges, far_arrived, 0)
    for c in range(16):
        hi, lo = split2(recv_f[pl.ds(c, ranges, stride=16), :])
        w_main[64 * c : 64 * c + ranges, 0:128] = hi
        w_main[64 * c : 64 * c + ranges, 128:256] = lo

    tall = 1024

    def far_rows(i, _):
        at = pl.ds(pl.multiple_of(i * tall, tall), tall)
        both = dot(count[at, :], w_main[...])
        far_main[at, :] = both[:, :128] + both[:, 128:]
        return 0

    lax.fori_loop(0, 4096 // tall, far_rows, 0)

    def near_arrived(o, _):
        exchange(send_n, recv_n, n_send, n_recv, o).wait()
        return 0

    lax.fori_loop(1, ranges, near_arrived, 0)
    for q in range(4):
        x = recv_n[pl.ds(16 + q, ranges, stride=24), :]
        for t in range(4):
            moved = pltpu.roll(x, 128 - TW * t, axis=1) if t else x
            at = 256 * t + 64 * q
            put_tail(pl.ds(at, ranges), moved)
    if ranges < 64:
        w_near[...] = jnp.zeros_like(w_near)
    for c in range(4):
        for l in range(5):
            row = 4 * l + c if l < 4 else 20 + c
            x = recv_n[pl.ds(row, ranges, stride=24), :]
            hi, lo = split2(x)
            w_near[64 * c : 64 * c + ranges, 128 * l : 128 * l + 128] = hi
            w_near[64 * c : 64 * c + ranges, QP + 128 * l : QP + 128 * l + 128] = lo

    def far_rows_tail(i, _):
        at = pl.ds(pl.multiple_of(i * tall, tall), tall)
        both = dot(count[at, :], w_tail[...])
        far_tail[at, :] = both + pltpu.roll(both, 128 - TW, axis=1)
        return 0

    lax.fori_loop(0, 4096 // tall, far_rows_tail, 0)

    for k in range(NCLS):
        m = jnp.concatenate(
            [ncount[pl.ds(k, 256, stride=16), :], ncount[pl.ds(4 + k, 256, stride=16), :]], axis=1
        ).astype(BF)
        hi, lo = split2(near_sum[k] + dot(m, w_near[:, 0:QP]) + dot(m, w_near[:, QP:]))
        parts[0:256, QP * k : QP * k + QP] = hi
        parts[256:512, QP * k : QP * k + QP] = lo

    group = 4
    local_sum[...] = jnp.zeros_like(local_sum)

    def far_class(i, _):
        his, los = [], []
        for k in range(group):
            at = pl.ds(i * group + k, 256, stride=16)
            for ref in (far_main, far_tail):
                hi, lo = split2(ref[at, :])
                his.append(hi)
                los.append(lo)
        high = jnp.concatenate(his, axis=1)
        at = pl.ds(pl.multiple_of(i * 256 * group, 256), 256 * group)
        both = dot(jnp.concatenate([high, jnp.concatenate(los, axis=1)], axis=0), f_hi[at, :])
        local_sum[...] += both[0:256] + both[256:512] + dot(high, f_lo[at, :])
        return 0

    lax.fori_loop(0, FCLS // group, far_class, 0)

    lh, ll = split2(local_sum[...])
    local_parts = jnp.concatenate([lh, ll], axis=0)
    back = []
    for n, (n0, w) in enumerate(((0, 256), (256, 256), (512, 128))):
        cols = slice(n0, n0 + w)
        both = dot(parts[...], n_hi[:, cols]) + dot(local_parts, t_hi[:, cols])
        total = both[0:256] + both[256:512]
        total = total + dot(parts[0:256, :], n_lo[:, cols]) + dot(lh, t_lo[:, cols])
        rs_send[:, :, cols] = total.reshape(4, BOX, w)
        for d in (2, 1, 3):
            copy = pltpu.make_async_remote_copy(
                src_ref=rs_send.at[lax.rem(h + d, 4), :, cols],
                dst_ref=rs_recv.at[d - 1, :, cols],
                send_sem=r_send.at[3 * n + d - 1],
                recv_sem=r_recv.at[3 * n + d - 1],
                device_id=helper(d),
                device_id_type=MESH,
            )
            copy.start()
            back.append(copy)
    for copy in back:
        copy.wait()
    total = rs_send[h] + rs_recv[0] + rs_recv[1] + rs_recv[2]
    out[...] = total[:, :QW]


def shards(sizes, multi, cheb, ghost, far_src, far_kind, far_count, near_src, near_kind, far_ops, near_ops, to_target):
    ranges = sizes[0] * sizes[1] * sizes[2]

    rows = ranges * 8
    vmem = pl.BlockSpec(memory_space=pltpu.VMEM)
    hbm = pl.BlockSpec(memory_space=pl.ANY)
    dma = pltpu.SemaphoreType.DMA
    return pl.pallas_call(
        functools.partial(evaluate, sizes),
        out_shape=jax.ShapeDtypeStruct((BOX, QW), F32),
        in_specs=[vmem] * 8 + [hbm] * 3,
        out_specs=vmem,
        scratch_shapes=[
            pltpu.VMEM((4, BOX, 128), F32),
            pltpu.VMEM((4, BOX, QP), F32),
            pltpu.VMEM((4, BOX, 512), I32),
            pltpu.VMEM((ranges, 16, 128), F32),
            pltpu.VMEM((ranges, 24, 128), F32),
            pltpu.VMEM((ranges * 16, 128), F32),
            pltpu.VMEM((ranges * 24, 128), F32),
            pltpu.VMEM((rows, 512), BF),
            pltpu.VMEM((rows, 512), BF),
            pltpu.VMEM((rows, 1024), BF),
            pltpu.VMEM((2560, 256), BF),
            pltpu.VMEM((128, 128), F32),
            pltpu.VMEM((256, 256), F32),
            pltpu.VMEM((256, 256), F32),
            pltpu.VMEM((4096, SW), BF),
            pltpu.VMEM((4096, 128), F32),
            pltpu.VMEM((SW, 256), BF),
            pltpu.VMEM((SW, 128), BF),
            pltpu.VMEM((256, 2 * QP), BF),
            pltpu.VMEM((4096, 128), F32),
            pltpu.VMEM((4096, 128), F32),
            pltpu.VMEM((FCLS, PW, PW), F32),
            pltpu.VMEM((NCLS, QW, QW), F32),
            pltpu.VMEM((PW, QW), F32),
            pltpu.VMEM((FCLS * 256, 256), BF),
            pltpu.VMEM((FCLS * 256, 256), BF),
            pltpu.VMEM((NCLS * QP, QP), BF),
            pltpu.VMEM((NCLS * QP, QP), BF),
            pltpu.VMEM((256, QP), BF),
            pltpu.VMEM((256, QP), BF),
            pltpu.VMEM((256, 256), F32),
            pltpu.VMEM((NCLS, 256, QP), F32),
            pltpu.VMEM((512, NCLS * QP), BF),
            pltpu.VMEM((4, BOX, QP), F32),
            pltpu.VMEM((3, BOX, QP), F32),
            dma((9,)),
            dma((9,)),
            dma((ranges,)),
            dma((ranges,)),
            dma((ranges,)),
            dma((ranges,)),
            dma((9,)),
            dma((9,)),
            dma((3,)),
        ],
        compiler_params=pltpu.CompilerParams(
            collective_id=0, has_side_effects=True, vmem_limit_bytes=60 * 1024 * 1024
        ),
        name="evaluate",
    )(
        multi,
        cheb,
        ghost,
        far_src,
        far_kind,
        far_count.reshape(1, BOX),
        near_src.T,
        near_kind.T,
        far_ops,
        near_ops,
        to_target,
    )


def solution(mesh, sizes=(4, 8, 2)):
    rows = P(("morton", "grp"), None)
    placed = (
        rows,
        rows,
        P("morton", None),
        rows,
        rows,
        P(("morton", "grp")),
        rows,
        rows,
        P(),
        P(),
        P(),
    )
    return jax.shard_map(
        functools.partial(shards, sizes), mesh=mesh, in_specs=placed, out_specs=rows, check_vma=False
    )
```

```python
import functools

import jax
import jax.numpy as jnp
from jax import lax
from jax.experimental import pallas as pl
from jax.experimental.pallas import tpu as pltpu
from jax.sharding import PartitionSpec as P

MESH = pl.DeviceIdType.MESH
BF = jnp.bfloat16
F32 = jnp.float32
I32 = jnp.int32

PW = 152
TW = PW - 128
QW = 560
QP = 640
FAR = 189
NEAR = 27
NEAR_AT = 192
CAP = 64
NCAP = 16
FCLS = 16
NCLS = 4
BOX = 64
KEYS = 160
SW = 1152


def split2(x):
    hi = x.astype(BF)
    return hi, (x - hi.astype(F32)).astype(BF)


def dot(a, b):
    return jnp.dot(a, b, preferred_element_type=F32)


def iota(shape, dim):
    return lax.broadcasted_iota(I32, shape, dim)


def evaluate(
    sizes,
    multi_in,
    cheb_in,
    ghost_in,
    far_src_in,
    far_kind_in,
    far_count_in,
    near_src_in,
    near_kind_in,
    far_ops,
    near_ops,
    to_target,
    out,
    multi,
    cheb,
    ghost,
    far_src,
    far_kind,
    far_count,
    near_src,
    near_kind,
    mall,
    call,
    iall,
    send_f,
    send_n,
    send_e,
    recv_f,
    recv_n,
    recv_e,
    pick_f,
    pick_n,
    pick_e,
    w_pick,
    turned,
    key_l,
    key_r,
    count,
    ncount,
    w_main,
    w_tail,
    w_near,
    far_main,
    far_tail,
    ops_f,
    ops_n,
    ops_t,
    f_hi,
    f_lo,
    n_hi,
    n_lo,
    t_hi,
    t_lo,
    local_sum,
    near_sum,
    total_far,
    parts,
    rs_send,
    rs_recv,
    fold,
    fold_recv,
    y_send,
    y_recv,
    f_send,
    f_recv,
    n_send,
    n_recv,
    e_send,
    e_recv,
    r_send,
    r_recv,
    load,
    small,
):
    xs, zs, cs = sizes
    ranges = xs * zs * cs
    me = lax.axis_index("morton")
    h = lax.axis_index("grp")
    my_x = lax.div(me, zs * cs)
    my_z = lax.rem(lax.div(me, cs), zs)
    my_c = lax.rem(me, cs)

    def helper(d):
        return (me, lax.rem(h + d, 4))

    across = []
    for zz in range(zs):
        dz = (zz + 1) // 2 if zz % 2 else zs - zz // 2
        across.append(lax.rem(my_z + dz, zs) * cs)

    def each_peer(visit):
        def some(i, first):
            dx, dc = lax.rem(i, xs), lax.div(i, xs)
            base = lax.rem(my_x + dx, xs) * (zs * cs) + lax.rem(my_c + dc, cs)
            for zz in range(first, zs):
                visit(i * zs + zz, base + across[zz])
            return 0

        some(0, 1)
        lax.fori_loop(1, xs * cs, lambda i, _: some(i, 0), 0)

    smalls = [
        pltpu.make_async_copy(src, dst, small.at[n])
        for n, (src, dst) in enumerate(
            (
                (multi_in, multi),
                (cheb_in, cheb),
                (far_src_in, far_src),
                (far_kind_in, far_kind),
                (far_count_in, far_count),
                (near_src_in, near_src),
                (near_kind_in, near_kind),
                (ghost_in, ghost),
            )
        )
    ]
    for copy in smalls:
        copy.start()
    loads = [
        pltpu.make_async_copy(far_ops, ops_f, load.at[0]),
        pltpu.make_async_copy(near_ops, ops_n, load.at[1]),
        pltpu.make_async_copy(to_target, ops_t, load.at[2]),
    ]
    barrier = pltpu.get_barrier_semaphore()
    for d in (2, 1, 3):
        pl.semaphore_signal(barrier, inc=1, device_id=helper(d), device_id_type=MESH)
    each_peer(
        lambda o, to: pl.semaphore_signal(barrier, inc=1, device_id=(to, h), device_id_type=MESH)
    )

    for copy in smalls:
        copy.wait()
    for copy in loads:
        copy.start()

    lane64 = iota((BOX, 128), 1)
    tail = jnp.concatenate([multi[:, 128:], jnp.zeros((BOX, 128 - TW), F32)], axis=1)
    rest = jnp.concatenate([cheb[:, 512:], jnp.zeros((BOX, QP - QW), F32)], axis=1)
    mall[h] = multi[:, 0:128]
    call[h, :, 0:512] = cheb[:, 0:512]
    call[h, :, 512:QP] = rest + pltpu.roll(tail, QW - 512, axis=1)
    turned[...] = jnp.zeros_like(turned)
    turned[0:NEAR, 0:BOX] = near_src[...].astype(F32)
    turned[32 : 32 + NEAR, 0:BOX] = near_kind[...].astype(F32)
    turned[64:65, 0:BOX] = far_count[...].astype(F32)
    near = turned[...].T[0:BOX, :]
    at_near = (lane64 >= 64) & (lane64 < 64 + NEAR)

    def second(far, shift):
        far = jnp.concatenate([far[:, 128:], jnp.zeros((BOX, 256 - FAR), I32)], axis=1)
        moved = pltpu.roll(near, shift, axis=1).astype(I32)
        return jnp.where(at_near, moved, jnp.where(lane64 < FAR - 128, far, 0))

    iall[h, :, 0:128] = far_src[:, 0:128]
    iall[h, :, 128:256] = second(far_src, 64)
    iall[h, :, 256:384] = far_kind[:, 0:128]
    live = pltpu.roll(near, 63, axis=1).astype(I32)
    iall[h, :, 384:512] = jnp.where(lane64 == 127, live, second(far_kind, 32))

    rows = ranges * 8
    step = min(128, rows)
    ghost_b = ghost[...].astype(F32).astype(BF)
    lane_c = iota((step, CAP), 1)
    sub = iota((step, CAP), 0) % 8
    lane256 = iota((step, 256), 1)
    low_half = (iota((step, 256), 0) % 8) < 4
    fifth = (iota((step, 256), 0) % 8) == 4

    def picker(at):
        own = ((iota((step, ranges), 0) + at) // 8) == iota((step, ranges), 1)
        each = dot(jnp.where(own, 1.0, 0.0).astype(BF), ghost_b)

        def chosen(slot):
            one = jnp.sum(jnp.where(lane_c == slot, each, 0.0), axis=1, keepdims=True)
            return lane256 == one.astype(I32)

        def put(ref, col, mask):
            ref[pl.ds(at, step), col : col + 256] = jnp.where(mask, 1.0, 0.0).astype(BF)

        return chosen, put

    def build_pick(i, _):
        chosen, put = picker(pl.multiple_of(i * step, step))
        put(pick_f, 0, chosen(16 * h + sub))
        put(pick_f, 256, chosen(16 * h + 8 + sub))
        return 0

    lax.fori_loop(0, rows // step, build_pick, 0)

    def build_late(i, _):
        chosen, put = picker(pl.multiple_of(i * step, step))
        near = chosen(4 * h + sub % 4)
        put(pick_n, 0, near & low_half)
        put(pick_n, 256, near & jnp.logical_not(low_half))
        for t in range(4):
            put(pick_e, 256 * t, chosen(16 * h + 4 * t + sub % 4) & low_half)
            put(pick_e, 256 * (5 + t), chosen(4 * h + t) & fifth)
        put(pick_e, 1024, near & low_half)
        return 0

    lax.fori_loop(0, rows // step, build_late, 0)

    for copy in loads:
        copy.wait()
    for ref in (f_hi, f_lo, n_hi, n_lo, t_hi, t_lo, near_sum, w_main, w_tail):
        ref[...] = jnp.zeros_like(ref)

    def split_far_op(k, _):
        hi, lo = split2(ops_f[k])
        at = pl.ds(pl.multiple_of(k * 256, 256), PW)
        f_hi[at, 0:PW] = hi
        f_lo[at, 0:PW] = lo
        return 0

    lax.fori_loop(0, FCLS, split_far_op, 0)

    def split_near_op(k, _):
        hi, lo = split2(ops_n[k])
        at = pl.ds(pl.multiple_of(k * QP, QP), QW)
        n_hi[at, 0:QW] = hi
        n_lo[at, 0:QW] = lo
        return 0

    lax.fori_loop(0, NCLS, split_near_op, 0)
    hi, lo = split2(ops_t[...])
    t_hi[0:PW, 0:QW] = hi
    t_lo[0:PW, 0:QW] = lo

    pl.semaphore_wait(barrier, ranges - 1 + 3)

    def to_helpers(k, ref):
        copies = []
        for d in (2, 1, 3):
            copies.append(
                pltpu.make_async_remote_copy(
                    src_ref=ref.at[h],
                    dst_ref=ref.at[h],
                    send_sem=y_send.at[3 * k + d - 1],
                    recv_sem=y_recv.at[3 * k + d - 1],
                    device_id=helper(d),
                    device_id_type=MESH,
                )
            )
        return copies

    y_copies = [to_helpers(0, mall), to_helpers(1, call), to_helpers(2, iall)]
    for copy in y_copies[0] + y_copies[2][1:] + y_copies[1] + y_copies[2][:1]:
        copy.start()

    lane = iota((BOX, 256), 1)

    def keys(g):
        src = iall[g, :, 0:256]
        kind = iall[g, :, 256:512]
        live = kind[:, 255:256]
        is_far = (lane < live) & (lane < FAR)
        is_near = (lane >= NEAR_AT) & (lane < NEAR_AT + NEAR)
        slot = src - 256
        s = slot >> 6
        c = slot & 63
        own = src < 256
        far_on = jnp.where(own, src >> 6, c >> 4) == h
        c = c & 15
        far_l = jnp.where(own, 128, (c >> 1) * 16) + kind
        far_r = jnp.where(own, src & 63, (c & 1) * 64 + s)
        slot = src - BOX
        s = slot >> 4
        c = slot & 15
        own = src < BOX
        near_on = jnp.where(own, g, c >> 2) == h
        c = c & 3
        near_l = jnp.where(own, 152, 144 + (c >> 1) * 4) + kind
        near_r = jnp.where(own, src, (c & 1) * 64 + s)
        on = (is_near & near_on) | (is_far & far_on)
        left = jnp.where(is_near, near_l, far_l)
        right = jnp.where(is_near, near_r, far_r)
        at = pl.ds(pl.multiple_of(g * BOX, BOX), BOX)
        key_l[at, :] = jnp.where(on, left, -1).astype(F32)
        key_r[at, :] = right.astype(F32)

    sub16 = iota((16, 256), 0).astype(F32).astype(BF)
    unroll = 8

    def count_box(b):
        kl = jnp.broadcast_to(key_l[pl.ds(b, 1), :], (16, 256)).astype(BF)
        kr = jnp.broadcast_to(key_r[pl.ds(b, 1), :], (16, 256)).astype(BF)
        one = jnp.ones((16, 256), BF)
        zero = jnp.zeros((16, 256), BF)
        left = jnp.concatenate(
            [
                jnp.where(kl == sub16 + jnp.asarray(16 * r, BF), one, zero)
                for r in range(KEYS // 16)
            ],
            axis=0,
        )
        right = jnp.concatenate(
            [jnp.where(kr == sub16 + jnp.asarray(16 * r, BF), one, zero) for r in range(8)],
            axis=0,
        )
        return lax.dot_general(
            left, right, (((1,), (1,)), ((), ())), preferred_element_type=F32
        )

    def count_block(g):
        def some(i, _):
            first = g * BOX + i * unroll
            found = [count_box(first + u) for u in range(unroll)]
            for u, both in enumerate(found):
                at = pl.ds(pl.multiple_of((first + u) * 16, 16), 16)
                for r in range(9):
                    count[at, 128 * r : 128 * r + 128] = both[16 * r : 16 * r + 16, :].astype(BF)
                ncount[at, :] = both[144:160, :]
            return 0

        lax.fori_loop(0, BOX // unroll, some, 0)

    keys(h)
    count_block(h)

    for copy in y_copies[0]:
        copy.wait()

    hi, lo = split2(mall[...].reshape(256, 128))
    w_pick[0:256, 0:128] = hi
    w_pick[0:256, 128:256] = lo
    messages = step // 8

    def pick_far(i, _):
        at = pl.multiple_of(i * step, step)
        to = pl.ds(i * messages, messages)
        for half in range(2):
            both = dot(pick_f[pl.ds(at, step), 256 * half : 256 * half + 256], w_pick[0:256, :])
            send_f[to, 8 * half : 8 * half + 8, :] = (both[:, :128] + both[:, 128:]).reshape(
                messages, 8, 128
            )
        return 0

    lax.fori_loop(0, rows // step, pick_far, 0)

    def block(s, n):
        return pl.ds(pl.multiple_of(s * n, n), n)

    def exchange(src, dst, s_sem, r_sem, o, to):
        n = src.shape[1]
        take = 5 if n == 8 else n
        return pltpu.make_async_remote_copy(
            src_ref=src.at[to, 0:take, :],
            dst_ref=dst.at[pl.ds(pl.multiple_of(me * n, n), take), :],
            send_sem=s_sem.at[o],
            recv_sem=r_sem.at[o],
            device_id=(to, h),
            device_id_type=MESH,
        )

    each_peer(lambda o, to: exchange(send_f, recv_f, f_send, f_recv, o, to).start())
    recv_f[block(me, 16), :] = send_f[me]

    own_cheb = jnp.concatenate([cheb[:, 0:512], rest], axis=1)
    own_cheb = jnp.concatenate([own_cheb, jnp.zeros((BOX, QP), F32)], axis=0)
    own_hi, own_lo = split2(own_cheb)
    mine = pl.ds(pl.multiple_of(h * BOX, BOX), BOX)
    for k in range(NCLS):
        m = ncount[pl.ds(h * 16 * BOX + 8 + k, BOX, stride=16), :].astype(BF)
        near_sum[k, mine, :] = dot(m, own_hi) + dot(m, own_lo)

    hi, lo = split2(multi[:, 0:128])
    w_main[1024:1088, 0:128] = hi
    w_main[1024:1088, 128:256] = lo

    def put_tail(at, x):
        high = x.astype(BF).astype(F32)
        keep = iota(x.shape, 1) < TW
        packed = jnp.where(keep, high, 0.0) + pltpu.roll(jnp.where(keep, x - high, 0.0), TW, axis=1)
        w_tail[at, :] = packed.astype(BF)

    put_tail(pl.ds(1024, BOX), tail)

    def other_block(d):
        g = lax.rem(h + d, 4)
        keys(g)
        count_block(g)

    y_copies[2][1].wait()
    other_block(3)
    y_copies[2][2].wait()
    other_block(1)

    for copy in y_copies[1]:
        copy.wait()

    lane_t = iota((256, 128), 1)
    last = call[:, :, 512:QP].reshape(256, 128)
    tails = jnp.where(lane_t < TW, pltpu.roll(last, 128 - (QW - 512), axis=1), 0.0)
    for t in range(4):
        hi, lo = split2(pltpu.roll(tails, TW * t, axis=1) if t else tails)
        w_pick[256 * (t + 1) : 256 * (t + 2), 0:128] = hi
        w_pick[256 * (t + 1) : 256 * (t + 2), 128:256] = lo
    ends = jnp.where(lane_t < 32, last, 0.0)
    blocks = [call[:, :, 128 * l : 128 * l + 128].reshape(256, 128) for l in range(4)]
    blocks.append(pltpu.roll(ends, 96, axis=1))
    ends = jnp.where((lane_t >= 32) & (lane_t < QW - 512), last, 0.0)
    for c in range(4):
        blocks.append(pltpu.roll(ends, (96 + 16 * c) % 128, axis=1) if c != 2 else ends)
    for l, part in enumerate(blocks):
        hi, lo = split2(part)
        w_pick[256 * (l + 5) : 256 * (l + 6), 0:128] = hi
        w_pick[256 * (l + 5) : 256 * (l + 6), 128:256] = lo

    def pick_ends(i, _):
        at = pl.multiple_of(i * step, step)
        both = dot(pick_e[pl.ds(at, step), 0:1024], w_pick[256:1280, :])
        both = both + dot(pick_e[pl.ds(at, step), 1024:2304], w_pick[256 * 9 : 256 * 14, :])
        send_e[pl.ds(i * messages, messages), :, :] = (both[:, :128] + both[:, 128:]).reshape(
            messages, 8, 128
        )
        return 0

    lax.fori_loop(0, rows // step, pick_ends, 0)

    each_peer(lambda o, to: exchange(send_e, recv_e, e_send, e_recv, o, to).start())
    recv_e[block(me, 8), :] = send_e[me]

    def pick_near(i, _):
        at = pl.multiple_of(i * step, step)
        to = pl.ds(i * messages, messages)
        near = pick_n[pl.ds(at, step), :]
        for half in range(2):
            both = dot(near, w_pick[256 * (5 + 2 * half) : 256 * (7 + 2 * half), :])
            send_n[to, 8 * half : 8 * half + 8, :] = (both[:, :128] + both[:, 128:]).reshape(
                messages, 8, 128
            )
        return 0

    lax.fori_loop(0, rows // step, pick_near, 0)

    each_peer(lambda o, to: exchange(send_n, recv_n, n_send, n_recv, o, to).start())
    recv_n[block(me, 16), :] = send_n[me]

    y_copies[2][0].wait()
    other_block(2)

    each_peer(lambda o, to: exchange(send_f, recv_f, f_send, f_recv, o, to).wait())
    for c in range(16):
        hi, lo = split2(recv_f[pl.ds(c, ranges, stride=16), :])
        w_main[64 * c : 64 * c + ranges, 0:128] = hi
        w_main[64 * c : 64 * c + ranges, 128:256] = lo

    tall = 1024

    def far_rows(i, _):
        at = pl.ds(pl.multiple_of(i * tall, tall), tall)
        both = dot(count[at, :], w_main[...])
        far_main[at, :] = both[:, :128] + both[:, 128:]
        return 0

    lax.fori_loop(0, 4096 // tall, far_rows, 0)

    each_peer(lambda o, to: exchange(send_e, recv_e, e_send, e_recv, o, to).wait())
    for q in range(4):
        x = recv_e[pl.ds(q, ranges, stride=8), :]
        for t in range(4):
            moved = pltpu.roll(x, 128 - TW * t, axis=1) if t else x
            at = 256 * t + 64 * q
            put_tail(pl.ds(at, ranges), moved)

    def far_rows_tail(i, _):
        at = pl.ds(pl.multiple_of(i * tall, tall), tall)
        both = dot(count[at, :], w_tail[...])
        far_tail[at, :] = both + pltpu.roll(both, 128 - TW, axis=1)
        return 0

    lax.fori_loop(0, 4096 // tall, far_rows_tail, 0)

    group = 4
    local_sum[...] = jnp.zeros_like(local_sum)

    def far_class(i, _):
        his, los = [], []
        for k in range(group):
            at = pl.ds(i * group + k, 256, stride=16)
            for ref in (far_main, far_tail):
                hi, lo = split2(ref[at, :])
                his.append(hi)
                los.append(lo)
        high = jnp.concatenate(his, axis=1)
        at = pl.ds(pl.multiple_of(i * 256 * group, 256), 256 * group)
        both = dot(jnp.concatenate([high, jnp.concatenate(los, axis=1)], axis=0), f_hi[at, :])
        local_sum[...] += both[0:256] + both[256:512] + dot(high, f_lo[at, :])
        return 0

    lax.fori_loop(0, FCLS // group, far_class, 0)

    lh, ll = split2(local_sum[...])
    left = jnp.concatenate([lh, ll, lh], axis=1)
    total_far[...] = dot(left, jnp.concatenate([t_hi[...], t_hi[...], t_lo[...]], axis=0))

    if ranges < 64:
        w_near[...] = jnp.zeros_like(w_near)

    def put_near(c, l, x):
        hi, lo = split2(x)
        w_near[64 * c : 64 * c + ranges, 128 * l : 128 * l + 128] = hi
        w_near[64 * c : 64 * c + ranges, QP + 128 * l : QP + 128 * l + 128] = lo

    fifths = recv_e[pl.ds(4, ranges, stride=8), :]
    lane_r = iota((ranges, 128), 1)
    for c in range(4):
        first = pltpu.roll(recv_e[pl.ds(c, ranges, stride=8), :], 32, axis=1)
        second = pltpu.roll(fifths, 32 - 16 * c, axis=1) if c < 2 else (
            pltpu.roll(fifths, 128 + 32 - 16 * c, axis=1) if c > 2 else fifths
        )
        x = jnp.where(lane_r < 32, first, jnp.where(lane_r < QW - 512, second, 0.0))
        put_near(c, 4, x)

    each_peer(lambda o, to: exchange(send_n, recv_n, n_send, n_recv, o, to).wait())
    for c in range(4):
        for l in range(4):
            put_near(c, l, recv_n[pl.ds(4 * l + c, ranges, stride=16), :])

    for k in range(NCLS):
        m = jnp.concatenate(
            [ncount[pl.ds(k, 256, stride=16), :], ncount[pl.ds(4 + k, 256, stride=16), :]], axis=1
        ).astype(BF)
        hi, lo = split2(near_sum[k] + dot(m, w_near[:, 0:QP]) + dot(m, w_near[:, QP:]))
        parts[0:256, QP * k : QP * k + QP] = hi
        parts[256:512, QP * k : QP * k + QP] = lo

    back = []
    for n, (n0, w) in enumerate(((512, 128), (0, 256), (256, 256))):
        cols = slice(n0, n0 + w)
        left = jnp.concatenate([parts[0:256, :], parts[256:512, :], parts[0:256, :]], axis=1)
        right = jnp.concatenate([n_hi[:, cols], n_hi[:, cols], n_lo[:, cols]], axis=0)
        total = (dot(left, right) + total_far[:, cols]).reshape(4, BOX, w)
        if n == 0:
            fold[...] = total[:, 0:32, :] + pltpu.roll(total[:, 32:64, :], 64, axis=2)
        else:
            rs_send[:, :, cols] = total
        for d in (2, 1, 3):
            to = lax.rem(h + d, 4)
            copy = pltpu.make_async_remote_copy(
                src_ref=rs_send.at[to, :, cols] if n else fold.at[to],
                dst_ref=rs_recv.at[d - 1, :, cols] if n else fold_recv.at[d - 1],
                send_sem=r_send.at[3 * n + d - 1],
                recv_sem=r_recv.at[3 * n + d - 1],
                device_id=helper(d),
                device_id_type=MESH,
            )
            copy.start()
            back.append(copy)
    for copy in back:
        copy.wait()
    out[:, 0:512] = rs_send[h] + rs_recv[0] + rs_recv[1] + rs_recv[2]
    total = fold[h] + fold_recv[0] + fold_recv[1] + fold_recv[2]
    out[0:32, 512:QW] = total[:, 0 : QW - 512]
    out[32:64, 512:QW] = pltpu.roll(total, 64, axis=1)[:, 0 : QW - 512]


def shards(sizes, multi, cheb, ghost, far_src, far_kind, far_count, near_src, near_kind, far_ops, near_ops, to_target):
    ranges = sizes[0] * sizes[1] * sizes[2]

    rows = ranges * 8
    vmem = pl.BlockSpec(memory_space=pltpu.VMEM)
    hbm = pl.BlockSpec(memory_space=pl.ANY)
    dma = pltpu.SemaphoreType.DMA
    return pl.pallas_call(
        functools.partial(evaluate, sizes),
        out_shape=pltpu.VMEM((BOX, QW), F32),
        in_specs=[hbm] * 11,
        out_specs=vmem,
        scratch_shapes=[
            pltpu.VMEM((BOX, PW), F32),
            pltpu.VMEM((BOX, QW), F32),
            pltpu.VMEM((ranges, CAP), I32),
            pltpu.VMEM((BOX, FAR), I32),
            pltpu.VMEM((BOX, FAR), I32),
            pltpu.VMEM((1, BOX), I32),
            pltpu.VMEM((NEAR, BOX), I32),
            pltpu.VMEM((NEAR, BOX), I32),
            pltpu.VMEM((4, BOX, 128), F32),
            pltpu.VMEM((4, BOX, QP), F32),
            pltpu.VMEM((4, BOX, 512), I32),
            pltpu.VMEM((ranges, 16, 128), F32),
            pltpu.VMEM((ranges, 16, 128), F32),
            pltpu.VMEM((ranges, 8, 128), F32),
            pltpu.VMEM((ranges * 16, 128), F32),
            pltpu.VMEM((ranges * 16, 128), F32),
            pltpu.VMEM((ranges * 8, 128), F32),
            pltpu.VMEM((rows, 512), BF),
            pltpu.VMEM((rows, 512), BF),
            pltpu.VMEM((rows, 2304), BF),
            pltpu.VMEM((256 * 14, 256), BF),
            pltpu.VMEM((128, 128), F32),
            pltpu.VMEM((256, 256), F32),
            pltpu.VMEM((256, 256), F32),
            pltpu.VMEM((4096, SW), BF),
            pltpu.VMEM((4096, 128), F32),
            pltpu.VMEM((SW, 256), BF),
            pltpu.VMEM((SW, 128), BF),
            pltpu.VMEM((256, 2 * QP), BF),
            pltpu.VMEM((4096, 128), F32),
            pltpu.VMEM((4096, 128), F32),
            pltpu.VMEM((FCLS, PW, PW), F32),
            pltpu.VMEM((NCLS, QW, QW), F32),
            pltpu.VMEM((PW, QW), F32),
            pltpu.VMEM((FCLS * 256, 256), BF),
            pltpu.VMEM((FCLS * 256, 256), BF),
            pltpu.VMEM((NCLS * QP, QP), BF),
            pltpu.VMEM((NCLS * QP, QP), BF),
            pltpu.VMEM((256, QP), BF),
            pltpu.VMEM((256, QP), BF),
            pltpu.VMEM((256, 256), F32),
            pltpu.VMEM((NCLS, 256, QP), F32),
            pltpu.VMEM((256, QP), F32),
            pltpu.VMEM((512, NCLS * QP), BF),
            pltpu.VMEM((4, BOX, 512), F32),
            pltpu.VMEM((3, BOX, 512), F32),
            pltpu.VMEM((4, 32, 128), F32),
            pltpu.VMEM((3, 32, 128), F32),
            dma((9,)),
            dma((9,)),
            dma((ranges,)),
            dma((ranges,)),
            dma((ranges,)),
            dma((ranges,)),
            dma((ranges,)),
            dma((ranges,)),
            dma((9,)),
            dma((9,)),
            dma((3,)),
            dma((8,)),
        ],
        compiler_params=pltpu.CompilerParams(
            collective_id=0, has_side_effects=True, vmem_limit_bytes=60 * 1024 * 1024
        ),
        name="evaluate",
    )(
        multi,
        cheb,
        ghost,
        far_src,
        far_kind,
        far_count.reshape(1, BOX),
        near_src.T,
        near_kind.T,
        far_ops,
        near_ops,
        to_target,
    )


def solution(mesh, sizes=(4, 8, 2)):
    rows = P(("morton", "grp"), None)
    placed = (
        rows,
        rows,
        P("morton", None),
        rows,
        rows,
        P(("morton", "grp")),
        rows,
        rows,
        P(),
        P(),
        P(),
    )
    return jax.shard_map(
        functools.partial(shards, sizes), mesh=mesh, in_specs=placed, out_specs=rows, check_vma=False
    )
```

```python
import functools

import jax
import jax.numpy as jnp
from jax import lax
from jax.experimental import pallas as pl
from jax.experimental.pallas import tpu as pltpu
from jax.sharding import PartitionSpec as P

MESH = pl.DeviceIdType.MESH
BF = jnp.bfloat16
F32 = jnp.float32
I32 = jnp.int32

PW = 152
TW = PW - 128
QW = 560
QP = 640
FAR = 189
NEAR = 27
NEAR_AT = 192
CAP = 64
NCAP = 16
FCLS = 16
NCLS = 4
BOX = 64
KEYS = 160
SW = 1152


def split2(x):
    hi = x.astype(BF)
    return hi, (x - hi.astype(F32)).astype(BF)


def dot(a, b):
    return jnp.dot(a, b, preferred_element_type=F32)


def iota(shape, dim):
    return lax.broadcasted_iota(I32, shape, dim)


def evaluate(
    sizes,
    multi_in,
    cheb_in,
    ghost_in,
    far_src_in,
    far_kind_in,
    far_count_in,
    near_src_in,
    near_kind_in,
    far_ops,
    near_ops,
    to_target,
    out,
    multi,
    cheb,
    ghost,
    far_src,
    far_kind,
    far_count,
    near_src,
    near_kind,
    mall,
    call,
    iall,
    send_f,
    send_n,
    send_e,
    recv_f,
    recv_n,
    recv_e,
    pick_f,
    pick_n,
    pick_e,
    w_pick,
    turned,
    key_l,
    key_r,
    count,
    ncount,
    w_main,
    w_tail,
    w_near,
    far_main,
    far_tail,
    ops_f,
    ops_n,
    ops_t,
    f_hi,
    f_lo,
    n_hi,
    n_lo,
    t_hi,
    t_lo,
    local_sum,
    near_sum,
    total_far,
    parts,
    rs_send,
    rs_recv,
    fold,
    fold_recv,
    y_send,
    y_recv,
    f_send,
    f_recv,
    n_send,
    n_recv,
    e_send,
    e_recv,
    r_send,
    r_recv,
    load,
    small,
):
    xs, zs, cs = sizes
    ranges = xs * zs * cs
    me = lax.axis_index("morton")
    h = lax.axis_index("grp")
    my_x = lax.div(me, zs * cs)
    my_z = lax.rem(lax.div(me, cs), zs)
    my_c = lax.rem(me, cs)

    def helper(d):
        return (me, lax.rem(h + d, 4))

    across = []
    for zz in range(zs):
        dz = (zz + 1) // 2 if zz % 2 else zs - zz // 2
        across.append(lax.rem(my_z + dz, zs) * cs)

    def each_peer(visit):
        def some(i, first):
            dx, dc = lax.rem(i, xs), lax.div(i, xs)
            base = lax.rem(my_x + dx, xs) * (zs * cs) + lax.rem(my_c + dc, cs)
            for zz in range(first, zs):
                visit(i * zs + zz, base + across[zz])
            return 0

        some(0, 1)
        lax.fori_loop(1, xs * cs, lambda i, _: some(i, 0), 0)

    smalls = [
        pltpu.make_async_copy(src, dst, small.at[n])
        for n, (src, dst) in enumerate(
            (
                (multi_in, multi),
                (cheb_in, cheb),
                (far_src_in, far_src),
                (far_kind_in, far_kind),
                (far_count_in, far_count),
                (near_src_in, near_src),
                (near_kind_in, near_kind),
                (ghost_in, ghost),
            )
        )
    ]
    for copy in smalls:
        copy.start()
    loads = [
        pltpu.make_async_copy(far_ops, ops_f, load.at[0]),
        pltpu.make_async_copy(near_ops, ops_n, load.at[1]),
        pltpu.make_async_copy(to_target, ops_t, load.at[2]),
    ]
    barrier = pltpu.get_barrier_semaphore()
    for d in (2, 1, 3):
        pl.semaphore_signal(barrier, inc=1, device_id=helper(d), device_id_type=MESH)
    each_peer(
        lambda o, to: pl.semaphore_signal(barrier, inc=1, device_id=(to, h), device_id_type=MESH)
    )

    for copy in smalls:
        copy.wait()
    for copy in loads:
        copy.start()

    lane64 = iota((BOX, 128), 1)
    tail = jnp.concatenate([multi[:, 128:], jnp.zeros((BOX, 128 - TW), F32)], axis=1)
    rest = jnp.concatenate([cheb[:, 512:], jnp.zeros((BOX, QP - QW), F32)], axis=1)
    mall[h] = multi[:, 0:128]
    call[h, :, 0:512] = cheb[:, 0:512]
    call[h, :, 512:QP] = rest + pltpu.roll(tail, QW - 512, axis=1)
    turned[...] = jnp.zeros_like(turned)
    turned[0:NEAR, 0:BOX] = near_src[...].astype(F32)
    turned[32 : 32 + NEAR, 0:BOX] = near_kind[...].astype(F32)
    turned[64:65, 0:BOX] = far_count[...].astype(F32)
    near = turned[...].T[0:BOX, :]
    at_near = (lane64 >= 64) & (lane64 < 64 + NEAR)

    def second(far, shift):
        far = jnp.concatenate([far[:, 128:], jnp.zeros((BOX, 256 - FAR), I32)], axis=1)
        moved = pltpu.roll(near, shift, axis=1).astype(I32)
        return jnp.where(at_near, moved, jnp.where(lane64 < FAR - 128, far, 0))

    iall[h, :, 0:128] = far_src[:, 0:128]
    iall[h, :, 128:256] = second(far_src, 64)
    iall[h, :, 256:384] = far_kind[:, 0:128]
    live = pltpu.roll(near, 63, axis=1).astype(I32)
    iall[h, :, 384:512] = jnp.where(lane64 == 127, live, second(far_kind, 32))

    rows = ranges * 8
    step = min(128, rows)
    ghost_b = ghost[...].astype(F32).astype(BF)
    lane_c = iota((step, CAP), 1)
    sub = iota((step, CAP), 0) % 8
    lane256 = iota((step, 256), 1)
    low_half = (iota((step, 256), 0) % 8) < 4
    fifth = (iota((step, 256), 0) % 8) == 4

    def picker(at):
        own = ((iota((step, ranges), 0) + at) // 8) == iota((step, ranges), 1)
        each = dot(jnp.where(own, 1.0, 0.0).astype(BF), ghost_b)

        def chosen(slot):
            one = jnp.sum(jnp.where(lane_c == slot, each, 0.0), axis=1, keepdims=True)
            return lane256 == one.astype(I32)

        def put(ref, col, mask):
            ref[pl.ds(at, step), col : col + 256] = jnp.where(mask, 1.0, 0.0).astype(BF)

        return chosen, put

    def build_pick(i, _):
        chosen, put = picker(pl.multiple_of(i * step, step))
        put(pick_f, 0, chosen(16 * h + sub))
        put(pick_f, 256, chosen(16 * h + 8 + sub))
        return 0

    lax.fori_loop(0, rows // step, build_pick, 0)

    def build_late(i, _):
        chosen, put = picker(pl.multiple_of(i * step, step))
        near = chosen(4 * h + sub % 4)
        put(pick_n, 0, near & low_half)
        put(pick_n, 256, near & jnp.logical_not(low_half))
        for t in range(4):
            put(pick_e, 256 * t, chosen(16 * h + 4 * t + sub % 4) & low_half)
            put(pick_e, 256 * (5 + t), chosen(4 * h + t) & fifth)
        put(pick_e, 1024, near & low_half)
        return 0

    lax.fori_loop(0, rows // step, build_late, 0)

    for copy in loads:
        copy.wait()
    n_hi[...] = jnp.zeros_like(n_hi)
    n_lo[...] = jnp.zeros_like(n_lo)

    def split_near_op(k, _):
        hi, lo = split2(ops_n[k])
        at = pl.ds(pl.multiple_of(k * QP, QP), QW)
        n_hi[at, 0:QW] = hi
        n_lo[at, 0:QW] = lo
        return 0

    lax.fori_loop(0, NCLS, split_near_op, 0)
    pl.semaphore_wait(barrier, ranges - 1 + 3)

    def to_helpers(k, ref):
        copies = []
        for d in (2, 1, 3):
            copies.append(
                pltpu.make_async_remote_copy(
                    src_ref=ref.at[h],
                    dst_ref=ref.at[h],
                    send_sem=y_send.at[3 * k + d - 1],
                    recv_sem=y_recv.at[3 * k + d - 1],
                    device_id=helper(d),
                    device_id_type=MESH,
                )
            )
        return copies

    y_copies = [to_helpers(0, mall), to_helpers(1, call), to_helpers(2, iall)]
    for copy in y_copies[0] + y_copies[2][1:] + y_copies[1] + y_copies[2][:1]:
        copy.start()

    for ref in (f_hi, f_lo, t_hi, t_lo, near_sum, w_main, w_tail):
        ref[...] = jnp.zeros_like(ref)

    def split_far_op(k, _):
        hi, lo = split2(ops_f[k])
        at = pl.ds(pl.multiple_of(k * 256, 256), PW)
        f_hi[at, 0:PW] = hi
        f_lo[at, 0:PW] = lo
        return 0

    lax.fori_loop(0, FCLS, split_far_op, 0)

    hi, lo = split2(ops_t[...])
    t_hi[0:PW, 0:QW] = hi
    t_lo[0:PW, 0:QW] = lo

    lane = iota((BOX, 256), 1)

    def keys(g):
        src = iall[g, :, 0:256]
        kind = iall[g, :, 256:512]
        live = kind[:, 255:256]
        is_far = (lane < live) & (lane < FAR)
        is_near = (lane >= NEAR_AT) & (lane < NEAR_AT + NEAR)
        slot = src - 256
        s = slot >> 6
        c = slot & 63
        own = src < 256
        far_on = jnp.where(own, src >> 6, c >> 4) == h
        c = c & 15
        far_l = jnp.where(own, 128, (c >> 1) * 16) + kind
        far_r = jnp.where(own, src & 63, (c & 1) * 64 + s)
        slot = src - BOX
        s = slot >> 4
        c = slot & 15
        own = src < BOX
        near_on = jnp.where(own, g, c >> 2) == h
        c = c & 3
        near_l = jnp.where(own, 152, 144 + (c >> 1) * 4) + kind
        near_r = jnp.where(own, src, (c & 1) * 64 + s)
        on = (is_near & near_on) | (is_far & far_on)
        left = jnp.where(is_near, near_l, far_l)
        right = jnp.where(is_near, near_r, far_r)
        at = pl.ds(pl.multiple_of(g * BOX, BOX), BOX)
        key_l[at, :] = jnp.where(on, left, -1).astype(F32)
        key_r[at, :] = right.astype(F32)

    sub16 = iota((16, 256), 0).astype(F32).astype(BF)
    unroll = 8

    def count_box(b):
        kl = jnp.broadcast_to(key_l[pl.ds(b, 1), :], (16, 256)).astype(BF)
        kr = jnp.broadcast_to(key_r[pl.ds(b, 1), :], (16, 256)).astype(BF)
        one = jnp.ones((16, 256), BF)
        zero = jnp.zeros((16, 256), BF)
        left = jnp.concatenate(
            [
                jnp.where(kl == sub16 + jnp.asarray(16 * r, BF), one, zero)
                for r in range(KEYS // 16)
            ],
            axis=0,
        )
        right = jnp.concatenate(
            [jnp.where(kr == sub16 + jnp.asarray(16 * r, BF), one, zero) for r in range(8)],
            axis=0,
        )
        return lax.dot_general(
            left, right, (((1,), (1,)), ((), ())), preferred_element_type=F32
        )

    def count_block(g):
        def some(i, _):
            first = g * BOX + i * unroll
            found = [count_box(first + u) for u in range(unroll)]
            for u, both in enumerate(found):
                at = pl.ds(pl.multiple_of((first + u) * 16, 16), 16)
                for r in range(9):
                    count[at, 128 * r : 128 * r + 128] = both[16 * r : 16 * r + 16, :].astype(BF)
                ncount[at, :] = both[144:160, :]
            return 0

        lax.fori_loop(0, BOX // unroll, some, 0)

    keys(h)
    count_block(h)

    for copy in y_copies[0]:
        copy.wait()

    hi, lo = split2(mall[...].reshape(256, 128))
    w_pick[0:256, 0:128] = hi
    w_pick[0:256, 128:256] = lo
    messages = step // 8

    def pick_far(i, _):
        at = pl.multiple_of(i * step, step)
        to = pl.ds(i * messages, messages)
        for half in range(2):
            both = dot(pick_f[pl.ds(at, step), 256 * half : 256 * half + 256], w_pick[0:256, :])
            send_f[to, 8 * half : 8 * half + 8, :] = (both[:, :128] + both[:, 128:]).reshape(
                messages, 8, 128
            )
        return 0

    lax.fori_loop(0, rows // step, pick_far, 0)

    def block(s, n):
        return pl.ds(pl.multiple_of(s * n, n), n)

    def exchange(src, dst, s_sem, r_sem, o, to):
        n = src.shape[1]
        take = 5 if n == 8 else n
        return pltpu.make_async_remote_copy(
            src_ref=src.at[to, 0:take, :],
            dst_ref=dst.at[pl.ds(pl.multiple_of(me * n, n), take), :],
            send_sem=s_sem.at[o],
            recv_sem=r_sem.at[o],
            device_id=(to, h),
            device_id_type=MESH,
        )

    each_peer(lambda o, to: exchange(send_f, recv_f, f_send, f_recv, o, to).start())
    recv_f[block(me, 16), :] = send_f[me]

    own_cheb = jnp.concatenate([cheb[:, 0:512], rest], axis=1)
    own_cheb = jnp.concatenate([own_cheb, jnp.zeros((BOX, QP), F32)], axis=0)
    own_hi, own_lo = split2(own_cheb)
    mine = pl.ds(pl.multiple_of(h * BOX, BOX), BOX)
    for k in range(NCLS):
        m = ncount[pl.ds(h * 16 * BOX + 8 + k, BOX, stride=16), :].astype(BF)
        near_sum[k, mine, :] = dot(m, own_hi) + dot(m, own_lo)

    hi, lo = split2(multi[:, 0:128])
    w_main[1024:1088, 0:128] = hi
    w_main[1024:1088, 128:256] = lo

    def put_tail(at, x):
        high = x.astype(BF).astype(F32)
        keep = iota(x.shape, 1) < TW
        packed = jnp.where(keep, high, 0.0) + pltpu.roll(jnp.where(keep, x - high, 0.0), TW, axis=1)
        w_tail[at, :] = packed.astype(BF)

    put_tail(pl.ds(1024, BOX), tail)

    def other_block(d):
        g = lax.rem(h + d, 4)
        keys(g)
        count_block(g)

    y_copies[2][1].wait()
    other_block(3)
    y_copies[2][2].wait()
    other_block(1)

    for copy in y_copies[1]:
        copy.wait()

    lane_t = iota((256, 128), 1)
    last = call[:, :, 512:QP].reshape(256, 128)
    tails = jnp.where(lane_t < TW, pltpu.roll(last, 128 - (QW - 512), axis=1), 0.0)
    for t in range(4):
        hi, lo = split2(pltpu.roll(tails, TW * t, axis=1) if t else tails)
        w_pick[256 * (t + 1) : 256 * (t + 2), 0:128] = hi
        w_pick[256 * (t + 1) : 256 * (t + 2), 128:256] = lo
    ends = jnp.where(lane_t < 32, last, 0.0)
    blocks = [call[:, :, 128 * l : 128 * l + 128].reshape(256, 128) for l in range(4)]
    blocks.append(pltpu.roll(ends, 96, axis=1))
    ends = jnp.where((lane_t >= 32) & (lane_t < QW - 512), last, 0.0)
    for c in range(4):
        blocks.append(pltpu.roll(ends, (96 + 16 * c) % 128, axis=1) if c != 2 else ends)
    for l, part in enumerate(blocks):
        hi, lo = split2(part)
        w_pick[256 * (l + 5) : 256 * (l + 6), 0:128] = hi
        w_pick[256 * (l + 5) : 256 * (l + 6), 128:256] = lo

    def pick_ends(i, _):
        at = pl.multiple_of(i * step, step)
        both = dot(pick_e[pl.ds(at, step), 0:1024], w_pick[256:1280, :])
        both = both + dot(pick_e[pl.ds(at, step), 1024:2304], w_pick[256 * 9 : 256 * 14, :])
        send_e[pl.ds(i * messages, messages), :, :] = (both[:, :128] + both[:, 128:]).reshape(
            messages, 8, 128
        )
        return 0

    lax.fori_loop(0, rows // step, pick_ends, 0)

    each_peer(lambda o, to: exchange(send_e, recv_e, e_send, e_recv, o, to).start())
    recv_e[block(me, 8), :] = send_e[me]

    def pick_near(i, _):
        at = pl.multiple_of(i * step, step)
        to = pl.ds(i * messages, messages)
        near = pick_n[pl.ds(at, step), :]
        for half in range(2):
            both = dot(near, w_pick[256 * (5 + 2 * half) : 256 * (7 + 2 * half), :])
            send_n[to, 8 * half : 8 * half + 8, :] = (both[:, :128] + both[:, 128:]).reshape(
                messages, 8, 128
            )
        return 0

    lax.fori_loop(0, rows // step, pick_near, 0)

    each_peer(lambda o, to: exchange(send_n, recv_n, n_send, n_recv, o, to).start())
    recv_n[block(me, 16), :] = send_n[me]

    y_copies[2][0].wait()
    other_block(2)

    each_peer(lambda o, to: exchange(send_f, recv_f, f_send, f_recv, o, to).wait())
    for c in range(16):
        hi, lo = split2(recv_f[pl.ds(c, ranges, stride=16), :])
        w_main[64 * c : 64 * c + ranges, 0:128] = hi
        w_main[64 * c : 64 * c + ranges, 128:256] = lo

    tall = 2048

    def far_rows(i, _):
        at = pl.ds(pl.multiple_of(i * tall, tall), tall)
        both = dot(count[at, :], w_main[...])
        far_main[at, :] = both[:, :128] + both[:, 128:]
        return 0

    lax.fori_loop(0, 4096 // tall, far_rows, 0)

    each_peer(lambda o, to: exchange(send_e, recv_e, e_send, e_recv, o, to).wait())
    for q in range(4):
        x = recv_e[pl.ds(q, ranges, stride=8), :]
        for t in range(4):
            moved = pltpu.roll(x, 128 - TW * t, axis=1) if t else x
            at = 256 * t + 64 * q
            put_tail(pl.ds(at, ranges), moved)

    def far_rows_tail(i, _):
        at = pl.ds(pl.multiple_of(i * tall, tall), tall)
        both = dot(count[at, :], w_tail[...])
        far_tail[at, :] = both + pltpu.roll(both, 128 - TW, axis=1)
        return 0

    lax.fori_loop(0, 4096 // tall, far_rows_tail, 0)

    group = 4
    local_sum[...] = jnp.zeros_like(local_sum)

    def far_class(i, _):
        his, los = [], []
        for k in range(group):
            at = pl.ds(i * group + k, 256, stride=16)
            for ref in (far_main, far_tail):
                hi, lo = split2(ref[at, :])
                his.append(hi)
                los.append(lo)
        high = jnp.concatenate(his, axis=1)
        at = pl.ds(pl.multiple_of(i * 256 * group, 256), 256 * group)
        both = dot(jnp.concatenate([high, jnp.concatenate(los, axis=1)], axis=0), f_hi[at, :])
        local_sum[...] += both[0:256] + both[256:512] + dot(high, f_lo[at, :])
        return 0

    lax.fori_loop(0, FCLS // group, far_class, 0)

    lh, ll = split2(local_sum[...])
    left = jnp.concatenate([lh, ll, lh], axis=1)
    total_far[...] = dot(left, jnp.concatenate([t_hi[...], t_hi[...], t_lo[...]], axis=0))

    if ranges < 64:
        w_near[...] = jnp.zeros_like(w_near)

    def put_near(c, l, x):
        hi, lo = split2(x)
        w_near[64 * c : 64 * c + ranges, 128 * l : 128 * l + 128] = hi
        w_near[64 * c : 64 * c + ranges, QP + 128 * l : QP + 128 * l + 128] = lo

    fifths = recv_e[pl.ds(4, ranges, stride=8), :]
    lane_r = iota((ranges, 128), 1)
    for c in range(4):
        first = pltpu.roll(recv_e[pl.ds(c, ranges, stride=8), :], 32, axis=1)
        second = pltpu.roll(fifths, 32 - 16 * c, axis=1) if c < 2 else (
            pltpu.roll(fifths, 128 + 32 - 16 * c, axis=1) if c > 2 else fifths
        )
        x = jnp.where(lane_r < 32, first, jnp.where(lane_r < QW - 512, second, 0.0))
        put_near(c, 4, x)

    each_peer(lambda o, to: exchange(send_n, recv_n, n_send, n_recv, o, to).wait())
    for c in range(4):
        for l in range(4):
            put_near(c, l, recv_n[pl.ds(4 * l + c, ranges, stride=16), :])

    for k in range(NCLS):
        m = jnp.concatenate(
            [ncount[pl.ds(k, 256, stride=16), :], ncount[pl.ds(4 + k, 256, stride=16), :]], axis=1
        ).astype(BF)
        hi, lo = split2(near_sum[k] + dot(m, w_near[:, 0:QP]) + dot(m, w_near[:, QP:]))
        parts[0:256, QP * k : QP * k + QP] = hi
        parts[256:512, QP * k : QP * k + QP] = lo

    back = []
    for n, (n0, w) in enumerate(((512, 128), (0, 256), (256, 256))):
        cols = slice(n0, n0 + w)
        right = jnp.concatenate([n_hi[:, cols], n_hi[:, cols], n_lo[:, cols]], axis=0)
        halves = []
        for m in (0, 128):
            high, low = parts[m : m + 128, :], parts[256 + m : 384 + m, :]
            halves.append(dot(jnp.concatenate([high, low, high], axis=1), right))
        total = jnp.concatenate(halves, axis=0)
        total = (total + total_far[:, cols]).reshape(4, BOX, w)
        if n == 0:
            fold[...] = total[:, 0:32, :] + pltpu.roll(total[:, 32:64, :], 64, axis=2)
        else:
            rs_send[:, :, cols] = total
        for d in (2, 1, 3):
            to = lax.rem(h + d, 4)
            copy = pltpu.make_async_remote_copy(
                src_ref=rs_send.at[to, :, cols] if n else fold.at[to],
                dst_ref=rs_recv.at[d - 1, :, cols] if n else fold_recv.at[d - 1],
                send_sem=r_send.at[3 * n + d - 1],
                recv_sem=r_recv.at[3 * n + d - 1],
                device_id=helper(d),
                device_id_type=MESH,
            )
            copy.start()
            back.append(copy)
    for copy in back:
        copy.wait()
    out[:, 0:512] = rs_send[h] + rs_recv[0] + rs_recv[1] + rs_recv[2]
    total = fold[h] + fold_recv[0] + fold_recv[1] + fold_recv[2]
    out[0:32, 512:QW] = total[:, 0 : QW - 512]
    out[32:64, 512:QW] = pltpu.roll(total, 64, axis=1)[:, 0 : QW - 512]


def shards(sizes, multi, cheb, ghost, far_src, far_kind, far_count, near_src, near_kind, far_ops, near_ops, to_target):
    ranges = sizes[0] * sizes[1] * sizes[2]

    rows = ranges * 8
    vmem = pl.BlockSpec(memory_space=pltpu.VMEM)
    hbm = pl.BlockSpec(memory_space=pl.ANY)
    dma = pltpu.SemaphoreType.DMA
    return pl.pallas_call(
        functools.partial(evaluate, sizes),
        out_shape=pltpu.VMEM((BOX, QW), F32),
        in_specs=[hbm] * 11,
        out_specs=vmem,
        scratch_shapes=[
            pltpu.VMEM((BOX, PW), F32),
            pltpu.VMEM((BOX, QW), F32),
            pltpu.VMEM((ranges, CAP), I32),
            pltpu.VMEM((BOX, FAR), I32),
            pltpu.VMEM((BOX, FAR), I32),
            pltpu.VMEM((1, BOX), I32),
            pltpu.VMEM((NEAR, BOX), I32),
            pltpu.VMEM((NEAR, BOX), I32),
            pltpu.VMEM((4, BOX, 128), F32),
            pltpu.VMEM((4, BOX, QP), F32),
            pltpu.VMEM((4, BOX, 512), I32),
            pltpu.VMEM((ranges, 16, 128), F32),
            pltpu.VMEM((ranges, 16, 128), F32),
            pltpu.VMEM((ranges, 8, 128), F32),
            pltpu.VMEM((ranges * 16, 128), F32),
            pltpu.VMEM((ranges * 16, 128), F32),
            pltpu.VMEM((ranges * 8, 128), F32),
            pltpu.VMEM((rows, 512), BF),
            pltpu.VMEM((rows, 512), BF),
            pltpu.VMEM((rows, 2304), BF),
            pltpu.VMEM((256 * 14, 256), BF),
            pltpu.VMEM((128, 128), F32),
            pltpu.VMEM((256, 256), F32),
            pltpu.VMEM((256, 256), F32),
            pltpu.VMEM((4096, SW), BF),
            pltpu.VMEM((4096, 128), F32),
            pltpu.VMEM((SW, 256), BF),
            pltpu.VMEM((SW, 128), BF),
            pltpu.VMEM((256, 2 * QP), BF),
            pltpu.VMEM((4096, 128), F32),
            pltpu.VMEM((4096, 128), F32),
            pltpu.VMEM((FCLS, PW, PW), F32),
            pltpu.VMEM((NCLS, QW, QW), F32),
            pltpu.VMEM((PW, QW), F32),
            pltpu.VMEM((FCLS * 256, 256), BF),
            pltpu.VMEM((FCLS * 256, 256), BF),
            pltpu.VMEM((NCLS * QP, QP), BF),
            pltpu.VMEM((NCLS * QP, QP), BF),
            pltpu.VMEM((256, QP), BF),
            pltpu.VMEM((256, QP), BF),
            pltpu.VMEM((256, 256), F32),
            pltpu.VMEM((NCLS, 256, QP), F32),
            pltpu.VMEM((256, QP), F32),
            pltpu.VMEM((512, NCLS * QP), BF),
            pltpu.VMEM((4, BOX, 512), F32),
            pltpu.VMEM((3, BOX, 512), F32),
            pltpu.VMEM((4, 32, 128), F32),
            pltpu.VMEM((3, 32, 128), F32),
            dma((9,)),
            dma((9,)),
            dma((ranges,)),
            dma((ranges,)),
            dma((ranges,)),
            dma((ranges,)),
            dma((ranges,)),
            dma((ranges,)),
            dma((9,)),
            dma((9,)),
            dma((3,)),
            dma((8,)),
        ],
        compiler_params=pltpu.CompilerParams(
            collective_id=0, has_side_effects=True, vmem_limit_bytes=60 * 1024 * 1024
        ),
        name="evaluate",
    )(
        multi,
        cheb,
        ghost,
        far_src,
        far_kind,
        far_count.reshape(1, BOX),
        near_src.T,
        near_kind.T,
        far_ops,
        near_ops,
        to_target,
    )


def solution(mesh, sizes=(4, 8, 2)):
    rows = P(("morton", "grp"), None)
    placed = (
        rows,
        rows,
        P("morton", None),
        rows,
        rows,
        P(("morton", "grp")),
        rows,
        rows,
        P(),
        P(),
        P(),
    )
    return jax.shard_map(
        functools.partial(shards, sizes), mesh=mesh, in_specs=placed, out_specs=rows, check_vma=False
    )
```

```python
import functools

import jax
import jax.numpy as jnp
from jax import lax
from jax.experimental import pallas as pl
from jax.experimental.pallas import tpu as pltpu
from jax.sharding import PartitionSpec as P

MESH = pl.DeviceIdType.MESH
BF = jnp.bfloat16
F32 = jnp.float32
I32 = jnp.int32

PW = 152
TW = PW - 128
QW = 560
QP = 640
NW = 768
FAR = 189
NEAR = 27
NEAR_AT = 192
CAP = 64
NCAP = 16
FCLS = 16
NCLS = 4
BOX = 64
KEYS = 160
SW = 1152


def split2(x):
    hi = x.astype(BF)
    return hi, (x - hi.astype(F32)).astype(BF)


def dot(a, b):
    return jnp.dot(a, b, preferred_element_type=F32)


def iota(shape, dim):
    return lax.broadcasted_iota(I32, shape, dim)


def evaluate(
    sizes,
    multi_in,
    cheb_in,
    ghost_in,
    far_src_in,
    far_kind_in,
    far_count_in,
    near_src_in,
    near_kind_in,
    far_ops,
    near_ops,
    to_target,
    out,
    multi,
    cheb,
    ghost,
    far_src,
    far_kind,
    far_count,
    near_src,
    near_kind,
    mall,
    call,
    iall,
    send_f,
    send_n,
    send_e,
    recv_f,
    recv_n,
    recv_e,
    pick_f,
    pick_n,
    pick_e,
    w_pick,
    turned,
    key_l,
    key_r,
    count,
    ncount,
    w_main,
    w_tail,
    w_near,
    far_main,
    far_tail,
    ops_f,
    ops_n,
    ops_t,
    f_hi,
    f_lo,
    n_hi,
    n_lo,
    t_hi,
    t_lo,
    local_sum,
    near_sum,
    total_far,
    parts,
    rs_send,
    rs_recv,
    fold,
    fold_recv,
    y_send,
    y_recv,
    f_send,
    f_recv,
    n_send,
    n_recv,
    e_send,
    e_recv,
    r_send,
    r_recv,
    load,
    small,
):
    xs, zs, cs = sizes
    ranges = xs * zs * cs
    me = lax.axis_index("morton")
    h = lax.axis_index("grp")
    my_x = lax.div(me, zs * cs)
    my_z = lax.rem(lax.div(me, cs), zs)
    my_c = lax.rem(me, cs)

    def helper(d):
        return (me, lax.rem(h + d, 4))

    across = []
    for zz in range(zs):
        dz = (zz + 1) // 2 if zz % 2 else zs - zz // 2
        across.append(lax.rem(my_z + dz, zs) * cs)

    def each_peer(visit):
        def some(i, first):
            dx, dc = lax.rem(i, xs), lax.div(i, xs)
            base = lax.rem(my_x + dx, xs) * (zs * cs) + lax.rem(my_c + dc, cs)
            for zz in range(first, zs):
                visit(i * zs + zz, base + across[zz])
            return 0

        some(0, 1)
        lax.fori_loop(1, xs * cs, lambda i, _: some(i, 0), 0)

    smalls = [
        pltpu.make_async_copy(src, dst, small.at[n])
        for n, (src, dst) in enumerate(
            (
                (multi_in, multi),
                (cheb_in, cheb),
                (far_src_in, far_src),
                (far_kind_in, far_kind),
                (far_count_in, far_count),
                (near_src_in, near_src),
                (near_kind_in, near_kind),
                (ghost_in, ghost),
            )
        )
    ]
    for copy in smalls:
        copy.start()
    loads = [
        pltpu.make_async_copy(far_ops, ops_f, load.at[0]),
        pltpu.make_async_copy(near_ops, ops_n, load.at[1]),
        pltpu.make_async_copy(to_target, ops_t, load.at[2]),
    ]
    barrier = pltpu.get_barrier_semaphore()
    for d in (2, 1, 3):
        pl.semaphore_signal(barrier, inc=1, device_id=helper(d), device_id_type=MESH)
    each_peer(
        lambda o, to: pl.semaphore_signal(barrier, inc=1, device_id=(to, h), device_id_type=MESH)
    )

    for copy in smalls:
        copy.wait()
    for copy in loads:
        copy.start()

    lane64 = iota((BOX, 128), 1)
    tail = jnp.concatenate([multi[:, 128:], jnp.zeros((BOX, 128 - TW), F32)], axis=1)
    rest = jnp.concatenate([cheb[:, 512:], jnp.zeros((BOX, QP - QW), F32)], axis=1)
    mall[h] = multi[:, 0:128]
    call[h, :, 0:512] = cheb[:, 0:512]
    call[h, :, 512:QP] = rest + pltpu.roll(tail, QW - 512, axis=1)
    turned[...] = jnp.zeros_like(turned)
    turned[0:NEAR, 0:BOX] = near_src[...].astype(F32)
    turned[32 : 32 + NEAR, 0:BOX] = near_kind[...].astype(F32)
    turned[64:65, 0:BOX] = far_count[...].astype(F32)
    near = turned[...].T[0:BOX, :]
    at_near = (lane64 >= 64) & (lane64 < 64 + NEAR)

    def second(far, shift):
        far = jnp.concatenate([far[:, 128:], jnp.zeros((BOX, 256 - FAR), I32)], axis=1)
        moved = pltpu.roll(near, shift, axis=1).astype(I32)
        return jnp.where(at_near, moved, jnp.where(lane64 < FAR - 128, far, 0))

    iall[h, :, 0:128] = far_src[:, 0:128]
    iall[h, :, 128:256] = second(far_src, 64)
    iall[h, :, 256:384] = far_kind[:, 0:128]
    live = pltpu.roll(near, 63, axis=1).astype(I32)
    iall[h, :, 384:512] = jnp.where(lane64 == 127, live, second(far_kind, 32))

    rows = ranges * 8
    step = min(128, rows)
    ghost_b = ghost[...].astype(F32).astype(BF)
    lane_c = iota((step, CAP), 1)
    sub = iota((step, CAP), 0) % 8
    lane256 = iota((step, 256), 1)
    low_half = (iota((step, 256), 0) % 8) < 4
    fifth = (iota((step, 256), 0) % 8) == 4

    def picker(at):
        own = ((iota((step, ranges), 0) + at) // 8) == iota((step, ranges), 1)
        each = dot(jnp.where(own, 1.0, 0.0).astype(BF), ghost_b)

        def chosen(slot):
            one = jnp.sum(jnp.where(lane_c == slot, each, 0.0), axis=1, keepdims=True)
            return lane256 == one.astype(I32)

        def put(ref, col, mask):
            ref[pl.ds(at, step), col : col + 256] = jnp.where(mask, 1.0, 0.0).astype(BF)

        return chosen, put

    def build_pick(i, _):
        chosen, put = picker(pl.multiple_of(i * step, step))
        put(pick_f, 0, chosen(16 * h + sub))
        put(pick_f, 256, chosen(16 * h + 8 + sub))
        return 0

    lax.fori_loop(0, rows // step, build_pick, 0)

    def build_late(i, _):
        chosen, put = picker(pl.multiple_of(i * step, step))
        near = chosen(4 * h + sub % 4)
        put(pick_n, 0, near & low_half)
        put(pick_n, 256, near & jnp.logical_not(low_half))
        for t in range(4):
            put(pick_e, 256 * t, chosen(16 * h + 4 * t + sub % 4) & low_half)
            put(pick_e, 256 * (5 + t), chosen(4 * h + t) & fifth)
        put(pick_e, 1024, near & low_half)
        return 0

    lax.fori_loop(0, rows // step, build_late, 0)

    for copy in loads:
        copy.wait()
    n_hi[...] = jnp.zeros_like(n_hi)
    n_lo[...] = jnp.zeros_like(n_lo)

    def split_near_op(k, _):
        hi, lo = split2(ops_n[k])
        at = pl.ds(pl.multiple_of(k * QP, QP), QW)
        n_hi[at, 0:QW] = hi
        n_lo[at, 0:QW] = lo
        return 0

    lax.fori_loop(0, NCLS, split_near_op, 0)
    pl.semaphore_wait(barrier, ranges - 1 + 3)

    def to_helpers(k, ref):
        copies = []
        for d in (2, 1, 3):
            copies.append(
                pltpu.make_async_remote_copy(
                    src_ref=ref.at[h],
                    dst_ref=ref.at[h],
                    send_sem=y_send.at[3 * k + d - 1],
                    recv_sem=y_recv.at[3 * k + d - 1],
                    device_id=helper(d),
                    device_id_type=MESH,
                )
            )
        return copies

    y_copies = [to_helpers(0, mall), to_helpers(1, call), to_helpers(2, iall)]
    for copy in y_copies[0] + y_copies[2][1:] + y_copies[1] + y_copies[2][:1]:
        copy.start()

    for ref in (f_hi, f_lo, t_hi, t_lo, near_sum, w_main, w_tail):
        ref[...] = jnp.zeros_like(ref)

    def split_far_op(k, _):
        hi, lo = split2(ops_f[k])
        at = pl.ds(pl.multiple_of(k * 256, 256), PW)
        f_hi[at, 0:PW] = hi
        f_lo[at, 0:PW] = lo
        return 0

    lax.fori_loop(0, FCLS, split_far_op, 0)

    hi, lo = split2(ops_t[...])
    t_hi[0:PW, 0:QW] = hi
    t_lo[0:PW, 0:QW] = lo

    lane = iota((BOX, 256), 1)

    def keys(g):
        src = iall[g, :, 0:256]
        kind = iall[g, :, 256:512]
        live = kind[:, 255:256]
        is_far = (lane < live) & (lane < FAR)
        is_near = (lane >= NEAR_AT) & (lane < NEAR_AT + NEAR)
        slot = src - 256
        s = slot >> 6
        c = slot & 63
        own = src < 256
        far_on = jnp.where(own, src >> 6, c >> 4) == h
        c = c & 15
        far_l = jnp.where(own, 128, (c >> 1) * 16) + kind
        far_r = jnp.where(own, src & 63, (c & 1) * 64 + s)
        slot = src - BOX
        s = slot >> 4
        c = slot & 15
        own = src < BOX
        near_on = jnp.where(own, g, c >> 2) == h
        c = c & 3
        near_l = jnp.where(own, 152, 144 + (c >> 1) * 4) + kind
        near_r = jnp.where(own, src, (c & 1) * 64 + s)
        on = (is_near & near_on) | (is_far & far_on)
        left = jnp.where(is_near, near_l, far_l)
        right = jnp.where(is_near, near_r, far_r)
        at = pl.ds(pl.multiple_of(g * BOX, BOX), BOX)
        key_l[at, :] = jnp.where(on, left, -1).astype(F32)
        key_r[at, :] = right.astype(F32)

    sub16 = iota((16, 256), 0).astype(F32).astype(BF)
    unroll = 8

    def count_box(b):
        kl = jnp.broadcast_to(key_l[pl.ds(b, 1), :], (16, 256)).astype(BF)
        kr = jnp.broadcast_to(key_r[pl.ds(b, 1), :], (16, 256)).astype(BF)
        one = jnp.ones((16, 256), BF)
        zero = jnp.zeros((16, 256), BF)
        left = jnp.concatenate(
            [
                jnp.where(kl == sub16 + jnp.asarray(16 * r, BF), one, zero)
                for r in range(KEYS // 16)
            ],
            axis=0,
        )
        right = jnp.concatenate(
            [jnp.where(kr == sub16 + jnp.asarray(16 * r, BF), one, zero) for r in range(8)],
            axis=0,
        )
        return lax.dot_general(
            left, right, (((1,), (1,)), ((), ())), preferred_element_type=F32
        )

    def count_block(g):
        def some(i, _):
            first = g * BOX + i * unroll
            found = [count_box(first + u) for u in range(unroll)]
            for u, both in enumerate(found):
                at = pl.ds(pl.multiple_of((first + u) * 16, 16), 16)
                for r in range(9):
                    count[at, 128 * r : 128 * r + 128] = both[16 * r : 16 * r + 16, :].astype(BF)
                ncount[at, :] = both[144:160, :]
            return 0

        lax.fori_loop(0, BOX // unroll, some, 0)

    keys(h)
    count_block(h)

    for copy in y_copies[0]:
        copy.wait()

    hi, lo = split2(mall[...].reshape(256, 128))
    w_pick[0:256, 0:128] = hi
    w_pick[0:256, 128:256] = lo
    messages = step // 8

    def pick_far(i, _):
        at = pl.multiple_of(i * step, step)
        to = pl.ds(i * messages, messages)
        for half in range(2):
            both = dot(pick_f[pl.ds(at, step), 256 * half : 256 * half + 256], w_pick[0:256, :])
            send_f[to, 8 * half : 8 * half + 8, :] = (both[:, :128] + both[:, 128:]).reshape(
                messages, 8, 128
            )
        return 0

    lax.fori_loop(0, rows // step, pick_far, 0)

    def block(s, n):
        return pl.ds(pl.multiple_of(s * n, n), n)

    def exchange(src, dst, s_sem, r_sem, o, to):
        n = src.shape[1]
        take = 5 if n == 8 else n
        return pltpu.make_async_remote_copy(
            src_ref=src.at[to, 0:take, :],
            dst_ref=dst.at[pl.ds(pl.multiple_of(me * n, n), take), :],
            send_sem=s_sem.at[o],
            recv_sem=r_sem.at[o],
            device_id=(to, h),
            device_id_type=MESH,
        )

    each_peer(lambda o, to: exchange(send_f, recv_f, f_send, f_recv, o, to).start())
    recv_f[block(me, 16), :] = send_f[me]

    own_cheb = jnp.concatenate([cheb[:, 0:512], rest], axis=1)
    own_cheb = jnp.concatenate([own_cheb, jnp.zeros((BOX, QP), F32)], axis=0)
    own_hi, own_lo = split2(own_cheb)
    mine = pl.ds(pl.multiple_of(h * BOX, BOX), BOX)
    for k in range(NCLS):
        m = ncount[pl.ds(h * 16 * BOX + 8 + k, BOX, stride=16), :].astype(BF)
        near_sum[k, mine, :] = dot(m, own_hi) + dot(m, own_lo)

    hi, lo = split2(multi[:, 0:128])
    w_main[1024:1088, 0:128] = hi
    w_main[1024:1088, 128:256] = lo

    def put_tail(at, x):
        high = x.astype(BF).astype(F32)
        keep = iota(x.shape, 1) < TW
        packed = jnp.where(keep, high, 0.0) + pltpu.roll(jnp.where(keep, x - high, 0.0), TW, axis=1)
        w_tail[at, :] = packed.astype(BF)

    put_tail(pl.ds(1024, BOX), tail)

    def other_block(d):
        g = lax.rem(h + d, 4)
        keys(g)
        count_block(g)

    y_copies[2][1].wait()
    other_block(3)
    y_copies[2][2].wait()
    other_block(1)

    for copy in y_copies[1]:
        copy.wait()

    lane_t = iota((256, 128), 1)
    last = call[:, :, 512:QP].reshape(256, 128)
    tails = jnp.where(lane_t < TW, pltpu.roll(last, 128 - (QW - 512), axis=1), 0.0)
    for t in range(4):
        hi, lo = split2(pltpu.roll(tails, TW * t, axis=1) if t else tails)
        w_pick[256 * (t + 1) : 256 * (t + 2), 0:128] = hi
        w_pick[256 * (t + 1) : 256 * (t + 2), 128:256] = lo
    ends = jnp.where(lane_t < 32, last, 0.0)
    blocks = [call[:, :, 128 * l : 128 * l + 128].reshape(256, 128) for l in range(4)]
    blocks.append(pltpu.roll(ends, 96, axis=1))
    ends = jnp.where((lane_t >= 32) & (lane_t < QW - 512), last, 0.0)
    for c in range(4):
        blocks.append(pltpu.roll(ends, (96 + 16 * c) % 128, axis=1) if c != 2 else ends)
    for l, part in enumerate(blocks):
        hi, lo = split2(part)
        w_pick[256 * (l + 5) : 256 * (l + 6), 0:128] = hi
        w_pick[256 * (l + 5) : 256 * (l + 6), 128:256] = lo

    def pick_ends(i, _):
        at = pl.multiple_of(i * step, step)
        both = dot(pick_e[pl.ds(at, step), 0:1024], w_pick[256:1280, :])
        both = both + dot(pick_e[pl.ds(at, step), 1024:2304], w_pick[256 * 9 : 256 * 14, :])
        send_e[pl.ds(i * messages, messages), :, :] = (both[:, :128] + both[:, 128:]).reshape(
            messages, 8, 128
        )
        return 0

    lax.fori_loop(0, rows // step, pick_ends, 0)

    each_peer(lambda o, to: exchange(send_e, recv_e, e_send, e_recv, o, to).start())
    recv_e[block(me, 8), :] = send_e[me]

    def pick_near(i, _):
        at = pl.multiple_of(i * step, step)
        to = pl.ds(i * messages, messages)
        near = pick_n[pl.ds(at, step), :]
        for half in range(2):
            both = dot(near, w_pick[256 * (5 + 2 * half) : 256 * (7 + 2 * half), :])
            send_n[to, 8 * half : 8 * half + 8, :] = (both[:, :128] + both[:, 128:]).reshape(
                messages, 8, 128
            )
        return 0

    lax.fori_loop(0, rows // step, pick_near, 0)

    each_peer(lambda o, to: exchange(send_n, recv_n, n_send, n_recv, o, to).start())
    recv_n[block(me, 16), :] = send_n[me]

    y_copies[2][0].wait()
    other_block(2)

    each_peer(lambda o, to: exchange(send_f, recv_f, f_send, f_recv, o, to).wait())
    for c in range(16):
        hi, lo = split2(recv_f[pl.ds(c, ranges, stride=16), :])
        w_main[64 * c : 64 * c + ranges, 0:128] = hi
        w_main[64 * c : 64 * c + ranges, 128:256] = lo

    tall = 1024

    def far_rows(i, _):
        at = pl.ds(pl.multiple_of(i * tall, tall), tall)
        both = dot(count[at, :], w_main[...])
        far_main[at, :] = both[:, :128] + both[:, 128:]
        return 0

    lax.fori_loop(0, 4096 // tall, far_rows, 0)

    each_peer(lambda o, to: exchange(send_e, recv_e, e_send, e_recv, o, to).wait())
    for q in range(4):
        x = recv_e[pl.ds(q, ranges, stride=8), :]
        for t in range(4):
            moved = pltpu.roll(x, 128 - TW * t, axis=1) if t else x
            at = 256 * t + 64 * q
            put_tail(pl.ds(at, ranges), moved)

    def far_rows_tail(i, _):
        at = pl.ds(pl.multiple_of(i * tall, tall), tall)
        both = dot(count[at, :], w_tail[...])
        far_tail[at, :] = both + pltpu.roll(both, 128 - TW, axis=1)
        return 0

    lax.fori_loop(0, 4096 // tall, far_rows_tail, 0)

    group = 4
    local_sum[...] = jnp.zeros_like(local_sum)

    def far_class(i, _):
        his, los = [], []
        for k in range(group):
            at = pl.ds(i * group + k, 256, stride=16)
            for ref in (far_main, far_tail):
                hi, lo = split2(ref[at, :])
                his.append(hi)
                los.append(lo)
        high = jnp.concatenate(his, axis=1)
        at = pl.ds(pl.multiple_of(i * 256 * group, 256), 256 * group)
        both = dot(jnp.concatenate([high, jnp.concatenate(los, axis=1)], axis=0), f_hi[at, :])
        local_sum[...] += both[0:256] + both[256:512] + dot(high, f_lo[at, :])
        return 0

    lax.fori_loop(0, FCLS // group, far_class, 0)

    lh, ll = split2(local_sum[...])
    left = jnp.concatenate([lh, ll, lh], axis=1)
    total_far[:, 0:QP] = dot(left, jnp.concatenate([t_hi[...], t_hi[...], t_lo[...]], axis=0))

    if ranges < 64:
        w_near[...] = jnp.zeros_like(w_near)

    def put_near(c, l, x):
        hi, lo = split2(x)
        w_near[64 * c : 64 * c + ranges, 128 * l : 128 * l + 128] = hi
        w_near[64 * c : 64 * c + ranges, QP + 128 * l : QP + 128 * l + 128] = lo

    fifths = recv_e[pl.ds(4, ranges, stride=8), :]
    lane_r = iota((ranges, 128), 1)
    for c in range(4):
        first = pltpu.roll(recv_e[pl.ds(c, ranges, stride=8), :], 32, axis=1)
        second = pltpu.roll(fifths, 32 - 16 * c, axis=1) if c < 2 else (
            pltpu.roll(fifths, 128 + 32 - 16 * c, axis=1) if c > 2 else fifths
        )
        x = jnp.where(lane_r < 32, first, jnp.where(lane_r < QW - 512, second, 0.0))
        put_near(c, 4, x)

    each_peer(lambda o, to: exchange(send_n, recv_n, n_send, n_recv, o, to).wait())
    for c in range(4):
        for l in range(4):
            put_near(c, l, recv_n[pl.ds(4 * l + c, ranges, stride=16), :])

    for k in range(NCLS):
        m = jnp.concatenate(
            [ncount[pl.ds(k, 256, stride=16), :], ncount[pl.ds(4 + k, 256, stride=16), :]], axis=1
        ).astype(BF)
        hi, lo = split2(near_sum[k] + dot(m, w_near[:, 0:QP]) + dot(m, w_near[:, QP:]))
        parts[0:256, QP * k : QP * k + QP] = hi
        parts[256:512, QP * k : QP * k + QP] = lo

    total_far[:, QP:NW] = jnp.zeros((256, NW - QP), F32)

    def folded(d):
        return pltpu.make_async_remote_copy(
            src_ref=fold.at[lax.rem(h + d, 4)],
            dst_ref=fold_recv.at[d - 1],
            send_sem=r_send.at[d - 1],
            recv_sem=r_recv.at[d - 1],
            device_id=helper(d),
            device_id_type=MESH,
        )

    def wide(n, d):
        cols = pl.ds(pl.multiple_of((n - 1) * 256, 256), 256)
        return pltpu.make_async_remote_copy(
            src_ref=rs_send.at[lax.rem(h + d, 4), :, cols],
            dst_ref=rs_recv.at[d - 1, :, cols],
            send_sem=r_send.at[3 * n + d - 1],
            recv_sem=r_recv.at[3 * n + d - 1],
            device_id=helper(d),
            device_id_type=MESH,
        )

    def give_back(n, _):
        at = pl.multiple_of(lax.rem(n + 2, 3) * 256, 256)
        cols = pl.ds(at, 256)
        right = jnp.concatenate([n_hi[:, cols], n_hi[:, cols], n_lo[:, cols]], axis=0)
        halves = []
        for m in (0, 128):
            high, low = parts[m : m + 128, :], parts[256 + m : 384 + m, :]
            halves.append(dot(jnp.concatenate([high, low, high], axis=1), right))
        total = jnp.concatenate(halves, axis=0)
        rs_send[:, :, cols] = (total + total_far[:, cols]).reshape(4, BOX, 256)

        @pl.when(n == 0)
        def _():
            narrow = rs_send[:, :, 512:640]
            fold[...] = narrow[:, 0:32, :] + pltpu.roll(narrow[:, 32:64, :], 64, axis=2)
            for d in (2, 1, 3):
                folded(d).start()

        @pl.when(n > 0)
        def _():
            for d in (2, 1, 3):
                wide(n, d).start()

        return 0

    lax.fori_loop(0, 3, give_back, 0)
    back = [folded(d) for d in (2, 1, 3)] + [wide(n, d) for n in (1, 2) for d in (2, 1, 3)]
    for copy in back:
        copy.wait()
    out[:, 0:512] = rs_send[h, :, 0:512] + rs_recv[0] + rs_recv[1] + rs_recv[2]
    total = fold[h] + fold_recv[0] + fold_recv[1] + fold_recv[2]
    out[0:32, 512:QW] = total[:, 0 : QW - 512]
    out[32:64, 512:QW] = pltpu.roll(total, 64, axis=1)[:, 0 : QW - 512]


def shards(sizes, multi, cheb, ghost, far_src, far_kind, far_count, near_src, near_kind, far_ops, near_ops, to_target):
    ranges = sizes[0] * sizes[1] * sizes[2]

    rows = ranges * 8
    vmem = pl.BlockSpec(memory_space=pltpu.VMEM)
    hbm = pl.BlockSpec(memory_space=pl.ANY)
    dma = pltpu.SemaphoreType.DMA
    return pl.pallas_call(
        functools.partial(evaluate, sizes),
        out_shape=pltpu.VMEM((BOX, QW), F32),
        in_specs=[hbm] * 11,
        out_specs=vmem,
        scratch_shapes=[
            pltpu.VMEM((BOX, PW), F32),
            pltpu.VMEM((BOX, QW), F32),
            pltpu.VMEM((ranges, CAP), I32),
            pltpu.VMEM((BOX, FAR), I32),
            pltpu.VMEM((BOX, FAR), I32),
            pltpu.VMEM((1, BOX), I32),
            pltpu.VMEM((NEAR, BOX), I32),
            pltpu.VMEM((NEAR, BOX), I32),
            pltpu.VMEM((4, BOX, 128), F32),
            pltpu.VMEM((4, BOX, QP), F32),
            pltpu.VMEM((4, BOX, 512), I32),
            pltpu.VMEM((ranges, 16, 128), F32),
            pltpu.VMEM((ranges, 16, 128), F32),
            pltpu.VMEM((ranges, 8, 128), F32),
            pltpu.VMEM((ranges * 16, 128), F32),
            pltpu.VMEM((ranges * 16, 128), F32),
            pltpu.VMEM((ranges * 8, 128), F32),
            pltpu.VMEM((rows, 512), BF),
            pltpu.VMEM((rows, 512), BF),
            pltpu.VMEM((rows, 2304), BF),
            pltpu.VMEM((256 * 14, 256), BF),
            pltpu.VMEM((128, 128), F32),
            pltpu.VMEM((256, 256), F32),
            pltpu.VMEM((256, 256), F32),
            pltpu.VMEM((4096, SW), BF),
            pltpu.VMEM((4096, 128), F32),
            pltpu.VMEM((SW, 256), BF),
            pltpu.VMEM((SW, 128), BF),
            pltpu.VMEM((256, 2 * QP), BF),
            pltpu.VMEM((4096, 128), F32),
            pltpu.VMEM((4096, 128), F32),
            pltpu.VMEM((FCLS, PW, PW), F32),
            pltpu.VMEM((NCLS, QW, QW), F32),
            pltpu.VMEM((PW, QW), F32),
            pltpu.VMEM((FCLS * 256, 256), BF),
            pltpu.VMEM((FCLS * 256, 256), BF),
            pltpu.VMEM((NCLS * QP, NW), BF),
            pltpu.VMEM((NCLS * QP, NW), BF),
            pltpu.VMEM((256, QP), BF),
            pltpu.VMEM((256, QP), BF),
            pltpu.VMEM((256, 256), F32),
            pltpu.VMEM((NCLS, 256, QP), F32),
            pltpu.VMEM((256, NW), F32),
            pltpu.VMEM((512, NCLS * QP), BF),
            pltpu.VMEM((4, BOX, NW), F32),
            pltpu.VMEM((3, BOX, 512), F32),
            pltpu.VMEM((4, 32, 128), F32),
            pltpu.VMEM((3, 32, 128), F32),
            dma((9,)),
            dma((9,)),
            dma((ranges,)),
            dma((ranges,)),
            dma((ranges,)),
            dma((ranges,)),
            dma((ranges,)),
            dma((ranges,)),
            dma((9,)),
            dma((9,)),
            dma((3,)),
            dma((8,)),
        ],
        compiler_params=pltpu.CompilerParams(
            collective_id=0, has_side_effects=True, vmem_limit_bytes=60 * 1024 * 1024
        ),
        name="evaluate",
    )(
        multi,
        cheb,
        ghost,
        far_src,
        far_kind,
        far_count.reshape(1, BOX),
        near_src.T,
        near_kind.T,
        far_ops,
        near_ops,
        to_target,
    )


def solution(mesh, sizes=(4, 8, 2)):
    rows = P(("morton", "grp"), None)
    placed = (
        rows,
        rows,
        P("morton", None),
        rows,
        rows,
        P(("morton", "grp")),
        rows,
        rows,
        P(),
        P(),
        P(),
    )
    return jax.shard_map(
        functools.partial(shards, sizes), mesh=mesh, in_specs=placed, out_specs=rows, check_vma=False
    )
```

```python
import functools

import jax
import jax.numpy as jnp
from jax import lax
from jax.experimental import pallas as pl
from jax.experimental.pallas import tpu as pltpu
from jax.sharding import PartitionSpec as P

MESH = pl.DeviceIdType.MESH
BF = jnp.bfloat16
F32 = jnp.float32
I32 = jnp.int32

PW = 152
TW = PW - 128
QW = 560
QP = 640
NW = 768
FAR = 189
NEAR = 27
NEAR_AT = 192
CAP = 64
NCAP = 16
FCLS = 16
NCLS = 4
BOX = 64
KEYS = 160
SW = 1152


def split2(x):
    hi = x.astype(BF)
    return hi, (x - hi.astype(F32)).astype(BF)


def dot(a, b):
    return jnp.dot(a, b, preferred_element_type=F32)


def iota(shape, dim):
    return lax.broadcasted_iota(I32, shape, dim)


def evaluate(
    sizes,
    multi_in,
    cheb_in,
    ghost_in,
    far_src_in,
    far_kind_in,
    far_count_in,
    near_src_in,
    near_kind_in,
    far_ops,
    near_ops,
    to_target,
    out,
    multi,
    cheb,
    ghost,
    far_src,
    far_kind,
    far_count,
    near_src,
    near_kind,
    mall,
    call,
    iall,
    send_f,
    send_n,
    send_e,
    recv_f,
    recv_n,
    recv_e,
    pick_f,
    pick_n,
    pick_e,
    w_pick,
    turned,
    key_l,
    key_r,
    count,
    ncount,
    w_main,
    w_tail,
    w_near,
    far_main,
    far_tail,
    ops_f,
    ops_n,
    ops_t,
    f_hi,
    f_lo,
    n_hi,
    n_lo,
    t_hi,
    t_lo,
    local_sum,
    near_sum,
    total_far,
    parts,
    rs_send,
    rs_recv,
    fold,
    fold_recv,
    y_send,
    y_recv,
    f_send,
    f_recv,
    n_send,
    n_recv,
    e_send,
    e_recv,
    r_send,
    r_recv,
    load,
    small,
):
    xs, zs, cs = sizes
    ranges = xs * zs * cs
    me = lax.axis_index("morton")
    h = lax.axis_index("grp")
    my_x = lax.div(me, zs * cs)
    my_z = lax.rem(lax.div(me, cs), zs)
    my_c = lax.rem(me, cs)

    def helper(d):
        return (me, lax.rem(h + d, 4))

    across = []
    for zz in range(zs):
        dz = (zz + 1) // 2 if zz % 2 else zs - zz // 2
        across.append(lax.rem(my_z + dz, zs) * cs)

    def each_peer(visit):
        def some(i, first):
            dx, dc = lax.rem(i, xs), lax.div(i, xs)
            base = lax.rem(my_x + dx, xs) * (zs * cs) + lax.rem(my_c + dc, cs)
            for zz in reversed(range(first, zs)):
                visit(i * zs + zz, base + across[zz])
            return 0

        lax.fori_loop(1, xs * cs, lambda i, _: some(xs * cs - i, 0), 0)
        some(0, 1)

    smalls = [
        pltpu.make_async_copy(src, dst, small.at[n])
        for n, (src, dst) in enumerate(
            (
                (multi_in, multi),
                (cheb_in, cheb),
                (far_src_in, far_src),
                (far_kind_in, far_kind),
                (far_count_in, far_count),
                (near_src_in, near_src),
                (near_kind_in, near_kind),
                (ghost_in, ghost),
            )
        )
    ]
    for copy in smalls:
        copy.start()
    loads = [
        pltpu.make_async_copy(far_ops, ops_f, load.at[0]),
        pltpu.make_async_copy(near_ops, ops_n, load.at[1]),
        pltpu.make_async_copy(to_target, ops_t, load.at[2]),
    ]
    barrier = pltpu.get_barrier_semaphore()
    for d in (2, 1, 3):
        pl.semaphore_signal(barrier, inc=1, device_id=helper(d), device_id_type=MESH)
    each_peer(
        lambda o, to: pl.semaphore_signal(barrier, inc=1, device_id=(to, h), device_id_type=MESH)
    )

    for copy in smalls:
        copy.wait()
    for copy in loads:
        copy.start()

    lane64 = iota((BOX, 128), 1)
    tail = jnp.concatenate([multi[:, 128:], jnp.zeros((BOX, 128 - TW), F32)], axis=1)
    rest = jnp.concatenate([cheb[:, 512:], jnp.zeros((BOX, QP - QW), F32)], axis=1)
    mall[h] = multi[:, 0:128]
    call[h, :, 0:512] = cheb[:, 0:512]
    call[h, :, 512:QP] = rest + pltpu.roll(tail, QW - 512, axis=1)
    turned[...] = jnp.zeros_like(turned)
    turned[0:NEAR, 0:BOX] = near_src[...].astype(F32)
    turned[32 : 32 + NEAR, 0:BOX] = near_kind[...].astype(F32)
    turned[64:65, 0:BOX] = far_count[...].astype(F32)
    near = turned[...].T[0:BOX, :]
    at_near = (lane64 >= 64) & (lane64 < 64 + NEAR)

    def second(far, shift):
        far = jnp.concatenate([far[:, 128:], jnp.zeros((BOX, 256 - FAR), I32)], axis=1)
        moved = pltpu.roll(near, shift, axis=1).astype(I32)
        return jnp.where(at_near, moved, jnp.where(lane64 < FAR - 128, far, 0))

    iall[h, :, 0:128] = far_src[:, 0:128]
    iall[h, :, 128:256] = second(far_src, 64)
    iall[h, :, 256:384] = far_kind[:, 0:128]
    live = pltpu.roll(near, 63, axis=1).astype(I32)
    iall[h, :, 384:512] = jnp.where(lane64 == 127, live, second(far_kind, 32))

    rows = ranges * 8
    step = min(128, rows)
    ghost_b = ghost[...].astype(F32).astype(BF)
    lane_c = iota((step, CAP), 1)
    sub = iota((step, CAP), 0) % 8
    lane256 = iota((step, 256), 1)
    low_half = (iota((step, 256), 0) % 8) < 4
    fifth = (iota((step, 256), 0) % 8) == 4

    def picker(at):
        own = ((iota((step, ranges), 0) + at) // 8) == iota((step, ranges), 1)
        each = dot(jnp.where(own, 1.0, 0.0).astype(BF), ghost_b)

        def chosen(slot):
            one = jnp.sum(jnp.where(lane_c == slot, each, 0.0), axis=1, keepdims=True)
            return lane256 == one.astype(I32)

        def put(ref, col, mask):
            ref[pl.ds(at, step), col : col + 256] = jnp.where(mask, 1.0, 0.0).astype(BF)

        return chosen, put

    def build_pick(i, _):
        chosen, put = picker(pl.multiple_of(i * step, step))
        put(pick_f, 0, chosen(16 * h + sub))
        put(pick_f, 256, chosen(16 * h + 8 + sub))
        return 0

    lax.fori_loop(0, rows // step, build_pick, 0)

    def build_late(i, _):
        chosen, put = picker(pl.multiple_of(i * step, step))
        near = chosen(4 * h + sub % 4)
        put(pick_n, 0, near & low_half)
        put(pick_n, 256, near & jnp.logical_not(low_half))
        for t in range(4):
            put(pick_e, 256 * t, chosen(16 * h + 4 * t + sub % 4) & low_half)
            put(pick_e, 256 * (5 + t), chosen(4 * h + t) & fifth)
        put(pick_e, 1024, near & low_half)
        return 0

    lax.fori_loop(0, rows // step, build_late, 0)

    for copy in loads:
        copy.wait()
    n_hi[...] = jnp.zeros_like(n_hi)
    n_lo[...] = jnp.zeros_like(n_lo)

    def split_near_op(k, _):
        hi, lo = split2(ops_n[k])
        at = pl.ds(pl.multiple_of(k * QP, QP), QW)
        n_hi[at, 0:QW] = hi
        n_lo[at, 0:QW] = lo
        return 0

    lax.fori_loop(0, NCLS, split_near_op, 0)
    pl.semaphore_wait(barrier, ranges - 1 + 3)

    def to_helpers(k, ref):
        copies = []
        for d in (2, 1, 3):
            copies.append(
                pltpu.make_async_remote_copy(
                    src_ref=ref.at[h],
                    dst_ref=ref.at[h],
                    send_sem=y_send.at[3 * k + d - 1],
                    recv_sem=y_recv.at[3 * k + d - 1],
                    device_id=helper(d),
                    device_id_type=MESH,
                )
            )
        return copies

    y_copies = [to_helpers(0, mall), to_helpers(1, call), to_helpers(2, iall)]
    for copy in y_copies[0] + y_copies[2][1:] + y_copies[1] + y_copies[2][:1]:
        copy.start()

    for ref in (f_hi, f_lo, t_hi, t_lo, near_sum, w_main, w_tail):
        ref[...] = jnp.zeros_like(ref)

    def split_far_op(k, _):
        hi, lo = split2(ops_f[k])
        at = pl.ds(pl.multiple_of(k * 256, 256), PW)
        f_hi[at, 0:PW] = hi
        f_lo[at, 0:PW] = lo
        return 0

    lax.fori_loop(0, FCLS, split_far_op, 0)

    hi, lo = split2(ops_t[...])
    t_hi[0:PW, 0:QW] = hi
    t_lo[0:PW, 0:QW] = lo

    lane = iota((BOX, 256), 1)

    def keys(g):
        src = iall[g, :, 0:256]
        kind = iall[g, :, 256:512]
        live = kind[:, 255:256]
        is_far = (lane < live) & (lane < FAR)
        is_near = (lane >= NEAR_AT) & (lane < NEAR_AT + NEAR)
        slot = src - 256
        s = slot >> 6
        c = slot & 63
        own = src < 256
        far_on = jnp.where(own, src >> 6, c >> 4) == h
        c = c & 15
        far_l = jnp.where(own, 128, (c >> 1) * 16) + kind
        far_r = jnp.where(own, src & 63, (c & 1) * 64 + s)
        slot = src - BOX
        s = slot >> 4
        c = slot & 15
        own = src < BOX
        near_on = jnp.where(own, g, c >> 2) == h
        c = c & 3
        near_l = jnp.where(own, 152, 144 + (c >> 1) * 4) + kind
        near_r = jnp.where(own, src, (c & 1) * 64 + s)
        on = (is_near & near_on) | (is_far & far_on)
        left = jnp.where(is_near, near_l, far_l)
        right = jnp.where(is_near, near_r, far_r)
        at = pl.ds(pl.multiple_of(g * BOX, BOX), BOX)
        key_l[at, :] = jnp.where(on, left, -1).astype(F32)
        key_r[at, :] = right.astype(F32)

    sub16 = iota((16, 256), 0).astype(F32).astype(BF)
    unroll = 8

    def count_box(b):
        kl = jnp.broadcast_to(key_l[pl.ds(b, 1), :], (16, 256)).astype(BF)
        kr = jnp.broadcast_to(key_r[pl.ds(b, 1), :], (16, 256)).astype(BF)
        one = jnp.ones((16, 256), BF)
        zero = jnp.zeros((16, 256), BF)
        left = jnp.concatenate(
            [
                jnp.where(kl == sub16 + jnp.asarray(16 * r, BF), one, zero)
                for r in range(KEYS // 16)
            ],
            axis=0,
        )
        right = jnp.concatenate(
            [jnp.where(kr == sub16 + jnp.asarray(16 * r, BF), one, zero) for r in range(8)],
            axis=0,
        )
        return lax.dot_general(
            left, right, (((1,), (1,)), ((), ())), preferred_element_type=F32
        )

    def count_block(g):
        def some(i, _):
            first = g * BOX + i * unroll
            found = [count_box(first + u) for u in range(unroll)]
            for u, both in enumerate(found):
                at = pl.ds(pl.multiple_of((first + u) * 16, 16), 16)
                for r in range(9):
                    count[at, 128 * r : 128 * r + 128] = both[16 * r : 16 * r + 16, :].astype(BF)
                ncount[at, :] = both[144:160, :]
            return 0

        lax.fori_loop(0, BOX // unroll, some, 0)

    keys(h)
    count_block(h)

    for copy in y_copies[0]:
        copy.wait()

    hi, lo = split2(mall[...].reshape(256, 128))
    w_pick[0:256, 0:128] = hi
    w_pick[0:256, 128:256] = lo
    messages = step // 8

    def pick_far(i, _):
        at = pl.multiple_of(i * step, step)
        to = pl.ds(i * messages, messages)
        for half in range(2):
            both = dot(pick_f[pl.ds(at, step), 256 * half : 256 * half + 256], w_pick[0:256, :])
            send_f[to, 8 * half : 8 * half + 8, :] = (both[:, :128] + both[:, 128:]).reshape(
                messages, 8, 128
            )
        return 0

    lax.fori_loop(0, rows // step, pick_far, 0)

    def block(s, n):
        return pl.ds(pl.multiple_of(s * n, n), n)

    def exchange(src, dst, s_sem, r_sem, o, to):
        n = src.shape[1]
        take = 5 if n == 8 else n
        return pltpu.make_async_remote_copy(
            src_ref=src.at[to, 0:take, :],
            dst_ref=dst.at[pl.ds(pl.multiple_of(me * n, n), take), :],
            send_sem=s_sem.at[o],
            recv_sem=r_sem.at[o],
            device_id=(to, h),
            device_id_type=MESH,
        )

    each_peer(lambda o, to: exchange(send_f, recv_f, f_send, f_recv, o, to).start())
    recv_f[block(me, 16), :] = send_f[me]

    own_cheb = jnp.concatenate([cheb[:, 0:512], rest], axis=1)
    own_cheb = jnp.concatenate([own_cheb, jnp.zeros((BOX, QP), F32)], axis=0)
    own_hi, own_lo = split2(own_cheb)
    mine = pl.ds(pl.multiple_of(h * BOX, BOX), BOX)
    for k in range(NCLS):
        m = ncount[pl.ds(h * 16 * BOX + 8 + k, BOX, stride=16), :].astype(BF)
        near_sum[k, mine, :] = dot(m, own_hi) + dot(m, own_lo)

    hi, lo = split2(multi[:, 0:128])
    w_main[1024:1088, 0:128] = hi
    w_main[1024:1088, 128:256] = lo

    def put_tail(at, x):
        high = x.astype(BF).astype(F32)
        keep = iota(x.shape, 1) < TW
        packed = jnp.where(keep, high, 0.0) + pltpu.roll(jnp.where(keep, x - high, 0.0), TW, axis=1)
        w_tail[at, :] = packed.astype(BF)

    put_tail(pl.ds(1024, BOX), tail)

    def other_block(d):
        g = lax.rem(h + d, 4)
        keys(g)
        count_block(g)

    y_copies[2][1].wait()
    other_block(3)
    y_copies[2][2].wait()
    other_block(1)

    for copy in y_copies[1]:
        copy.wait()

    lane_t = iota((256, 128), 1)
    last = call[:, :, 512:QP].reshape(256, 128)
    tails = jnp.where(lane_t < TW, pltpu.roll(last, 128 - (QW - 512), axis=1), 0.0)
    for t in range(4):
        hi, lo = split2(pltpu.roll(tails, TW * t, axis=1) if t else tails)
        w_pick[256 * (t + 1) : 256 * (t + 2), 0:128] = hi
        w_pick[256 * (t + 1) : 256 * (t + 2), 128:256] = lo
    ends = jnp.where(lane_t < 32, last, 0.0)
    blocks = [call[:, :, 128 * l : 128 * l + 128].reshape(256, 128) for l in range(4)]
    blocks.append(pltpu.roll(ends, 96, axis=1))
    ends = jnp.where((lane_t >= 32) & (lane_t < QW - 512), last, 0.0)
    for c in range(4):
        blocks.append(pltpu.roll(ends, (96 + 16 * c) % 128, axis=1) if c != 2 else ends)
    for l, part in enumerate(blocks):
        hi, lo = split2(part)
        w_pick[256 * (l + 5) : 256 * (l + 6), 0:128] = hi
        w_pick[256 * (l + 5) : 256 * (l + 6), 128:256] = lo

    def pick_ends(i, _):
        at = pl.multiple_of(i * step, step)
        both = dot(pick_e[pl.ds(at, step), 0:1024], w_pick[256:1280, :])
        both = both + dot(pick_e[pl.ds(at, step), 1024:2304], w_pick[256 * 9 : 256 * 14, :])
        send_e[pl.ds(i * messages, messages), :, :] = (both[:, :128] + both[:, 128:]).reshape(
            messages, 8, 128
        )
        return 0

    lax.fori_loop(0, rows // step, pick_ends, 0)

    each_peer(lambda o, to: exchange(send_e, recv_e, e_send, e_recv, o, to).start())
    recv_e[block(me, 8), :] = send_e[me]

    def pick_near(i, _):
        at = pl.multiple_of(i * step, step)
        to = pl.ds(i * messages, messages)
        near = pick_n[pl.ds(at, step), :]
        for half in range(2):
            both = dot(near, w_pick[256 * (5 + 2 * half) : 256 * (7 + 2 * half), :])
            send_n[to, 8 * half : 8 * half + 8, :] = (both[:, :128] + both[:, 128:]).reshape(
                messages, 8, 128
            )
        return 0

    lax.fori_loop(0, rows // step, pick_near, 0)

    each_peer(lambda o, to: exchange(send_n, recv_n, n_send, n_recv, o, to).start())
    recv_n[block(me, 16), :] = send_n[me]

    y_copies[2][0].wait()
    other_block(2)

    each_peer(lambda o, to: exchange(send_f, recv_f, f_send, f_recv, o, to).wait())
    for c in range(16):
        hi, lo = split2(recv_f[pl.ds(c, ranges, stride=16), :])
        w_main[64 * c : 64 * c + ranges, 0:128] = hi
        w_main[64 * c : 64 * c + ranges, 128:256] = lo

    tall = 1024

    def far_rows(i, _):
        at = pl.ds(pl.multiple_of(i * tall, tall), tall)
        both = dot(count[at, :], w_main[...])
        far_main[at, :] = both[:, :128] + both[:, 128:]
        return 0

    lax.fori_loop(0, 4096 // tall, far_rows, 0)

    each_peer(lambda o, to: exchange(send_e, recv_e, e_send, e_recv, o, to).wait())
    for q in range(4):
        x = recv_e[pl.ds(q, ranges, stride=8), :]
        for t in range(4):
            moved = pltpu.roll(x, 128 - TW * t, axis=1) if t else x
            at = 256 * t + 64 * q
            put_tail(pl.ds(at, ranges), moved)

    def far_rows_tail(i, _):
        at = pl.ds(pl.multiple_of(i * tall, tall), tall)
        both = dot(count[at, :], w_tail[...])
        far_tail[at, :] = both + pltpu.roll(both, 128 - TW, axis=1)
        return 0

    lax.fori_loop(0, 4096 // tall, far_rows_tail, 0)

    group = 4
    local_sum[...] = jnp.zeros_like(local_sum)

    def far_class(i, _):
        his, los = [], []
        for k in range(group):
            at = pl.ds(i * group + k, 256, stride=16)
            for ref in (far_main, far_tail):
                hi, lo = split2(ref[at, :])
                his.append(hi)
                los.append(lo)
        high = jnp.concatenate(his, axis=1)
        at = pl.ds(pl.multiple_of(i * 256 * group, 256), 256 * group)
        both = dot(jnp.concatenate([high, jnp.concatenate(los, axis=1)], axis=0), f_hi[at, :])
        local_sum[...] += both[0:256] + both[256:512] + dot(high, f_lo[at, :])
        return 0

    lax.fori_loop(0, FCLS // group, far_class, 0)

    lh, ll = split2(local_sum[...])
    left = jnp.concatenate([lh, ll, lh], axis=1)
    total_far[:, 0:QP] = dot(left, jnp.concatenate([t_hi[...], t_hi[...], t_lo[...]], axis=0))

    if ranges < 64:
        w_near[...] = jnp.zeros_like(w_near)

    def put_near(c, l, x):
        hi, lo = split2(x)
        w_near[64 * c : 64 * c + ranges, 128 * l : 128 * l + 128] = hi
        w_near[64 * c : 64 * c + ranges, QP + 128 * l : QP + 128 * l + 128] = lo

    fifths = recv_e[pl.ds(4, ranges, stride=8), :]
    lane_r = iota((ranges, 128), 1)
    for c in range(4):
        first = pltpu.roll(recv_e[pl.ds(c, ranges, stride=8), :], 32, axis=1)
        second = pltpu.roll(fifths, 32 - 16 * c, axis=1) if c < 2 else (
            pltpu.roll(fifths, 128 + 32 - 16 * c, axis=1) if c > 2 else fifths
        )
        x = jnp.where(lane_r < 32, first, jnp.where(lane_r < QW - 512, second, 0.0))
        put_near(c, 4, x)

    each_peer(lambda o, to: exchange(send_n, recv_n, n_send, n_recv, o, to).wait())
    for c in range(4):
        for l in range(4):
            put_near(c, l, recv_n[pl.ds(4 * l + c, ranges, stride=16), :])

    for k in range(NCLS):
        m = jnp.concatenate(
            [ncount[pl.ds(k, 256, stride=16), :], ncount[pl.ds(4 + k, 256, stride=16), :]], axis=1
        ).astype(BF)
        hi, lo = split2(near_sum[k] + dot(m, w_near[:, 0:QP]) + dot(m, w_near[:, QP:]))
        parts[0:256, QP * k : QP * k + QP] = hi
        parts[256:512, QP * k : QP * k + QP] = lo

    total_far[:, QP:NW] = jnp.zeros((256, NW - QP), F32)

    def folded(d):
        return pltpu.make_async_remote_copy(
            src_ref=fold.at[lax.rem(h + d, 4)],
            dst_ref=fold_recv.at[d - 1],
            send_sem=r_send.at[d - 1],
            recv_sem=r_recv.at[d - 1],
            device_id=helper(d),
            device_id_type=MESH,
        )

    def wide(n, d):
        cols = pl.ds(pl.multiple_of((n - 1) * 256, 256), 256)
        return pltpu.make_async_remote_copy(
            src_ref=rs_send.at[lax.rem(h + d, 4), :, cols],
            dst_ref=rs_recv.at[d - 1, :, cols],
            send_sem=r_send.at[3 * n + d - 1],
            recv_sem=r_recv.at[3 * n + d - 1],
            device_id=helper(d),
            device_id_type=MESH,
        )

    def give_back(n, _):
        at = pl.multiple_of(lax.rem(n + 2, 3) * 256, 256)
        cols = pl.ds(at, 256)
        right = jnp.concatenate([n_hi[:, cols], n_hi[:, cols], n_lo[:, cols]], axis=0)
        halves = []
        for m in (0, 128):
            high, low = parts[m : m + 128, :], parts[256 + m : 384 + m, :]
            halves.append(dot(jnp.concatenate([high, low, high], axis=1), right))
        total = jnp.concatenate(halves, axis=0)
        rs_send[:, :, cols] = (total + total_far[:, cols]).reshape(4, BOX, 256)

        @pl.when(n == 0)
        def _():
            narrow = rs_send[:, :, 512:640]
            fold[...] = narrow[:, 0:32, :] + pltpu.roll(narrow[:, 32:64, :], 64, axis=2)
            for d in (2, 1, 3):
                folded(d).start()

        @pl.when(n > 0)
        def _():
            for d in (2, 1, 3):
                wide(n, d).start()

        return 0

    lax.fori_loop(0, 3, give_back, 0)
    back = [folded(d) for d in (2, 1, 3)] + [wide(n, d) for n in (1, 2) for d in (2, 1, 3)]
    for copy in back:
        copy.wait()
    out[:, 0:512] = rs_send[h, :, 0:512] + rs_recv[0] + rs_recv[1] + rs_recv[2]
    total = fold[h] + fold_recv[0] + fold_recv[1] + fold_recv[2]
    out[0:32, 512:QW] = total[:, 0 : QW - 512]
    out[32:64, 512:QW] = pltpu.roll(total, 64, axis=1)[:, 0 : QW - 512]


def shards(sizes, multi, cheb, ghost, far_src, far_kind, far_count, near_src, near_kind, far_ops, near_ops, to_target):
    ranges = sizes[0] * sizes[1] * sizes[2]

    rows = ranges * 8
    vmem = pl.BlockSpec(memory_space=pltpu.VMEM)
    hbm = pl.BlockSpec(memory_space=pl.ANY)
    dma = pltpu.SemaphoreType.DMA
    return pl.pallas_call(
        functools.partial(evaluate, sizes),
        out_shape=pltpu.VMEM((BOX, QW), F32),
        in_specs=[hbm] * 11,
        out_specs=vmem,
        scratch_shapes=[
            pltpu.VMEM((BOX, PW), F32),
            pltpu.VMEM((BOX, QW), F32),
            pltpu.VMEM((ranges, CAP), I32),
            pltpu.VMEM((BOX, FAR), I32),
            pltpu.VMEM((BOX, FAR), I32),
            pltpu.VMEM((1, BOX), I32),
            pltpu.VMEM((NEAR, BOX), I32),
            pltpu.VMEM((NEAR, BOX), I32),
            pltpu.VMEM((4, BOX, 128), F32),
            pltpu.VMEM((4, BOX, QP), F32),
            pltpu.VMEM((4, BOX, 512), I32),
            pltpu.VMEM((ranges, 16, 128), F32),
            pltpu.VMEM((ranges, 16, 128), F32),
            pltpu.VMEM((ranges, 8, 128), F32),
            pltpu.VMEM((ranges * 16, 128), F32),
            pltpu.VMEM((ranges * 16, 128), F32),
            pltpu.VMEM((ranges * 8, 128), F32),
            pltpu.VMEM((rows, 512), BF),
            pltpu.VMEM((rows, 512), BF),
            pltpu.VMEM((rows, 2304), BF),
            pltpu.VMEM((256 * 14, 256), BF),
            pltpu.VMEM((128, 128), F32),
            pltpu.VMEM((256, 256), F32),
            pltpu.VMEM((256, 256), F32),
            pltpu.VMEM((4096, SW), BF),
            pltpu.VMEM((4096, 128), F32),
            pltpu.VMEM((SW, 256), BF),
            pltpu.VMEM((SW, 128), BF),
            pltpu.VMEM((256, 2 * QP), BF),
            pltpu.VMEM((4096, 128), F32),
            pltpu.VMEM((4096, 128), F32),
            pltpu.VMEM((FCLS, PW, PW), F32),
            pltpu.VMEM((NCLS, QW, QW), F32),
            pltpu.VMEM((PW, QW), F32),
            pltpu.VMEM((FCLS * 256, 256), BF),
            pltpu.VMEM((FCLS * 256, 256), BF),
            pltpu.VMEM((NCLS * QP, NW), BF),
            pltpu.VMEM((NCLS * QP, NW), BF),
            pltpu.VMEM((256, QP), BF),
            pltpu.VMEM((256, QP), BF),
            pltpu.VMEM((256, 256), F32),
            pltpu.VMEM((NCLS, 256, QP), F32),
            pltpu.VMEM((256, NW), F32),
            pltpu.VMEM((512, NCLS * QP), BF),
            pltpu.VMEM((4, BOX, NW), F32),
            pltpu.VMEM((3, BOX, 512), F32),
            pltpu.VMEM((4, 32, 128), F32),
            pltpu.VMEM((3, 32, 128), F32),
            dma((9,)),
            dma((9,)),
            dma((ranges,)),
            dma((ranges,)),
            dma((ranges,)),
            dma((ranges,)),
            dma((ranges,)),
            dma((ranges,)),
            dma((9,)),
            dma((9,)),
            dma((3,)),
            dma((8,)),
        ],
        compiler_params=pltpu.CompilerParams(
            collective_id=0, has_side_effects=True, vmem_limit_bytes=60 * 1024 * 1024
        ),
        name="evaluate",
    )(
        multi,
        cheb,
        ghost,
        far_src,
        far_kind,
        far_count.reshape(1, BOX),
        near_src.T,
        near_kind.T,
        far_ops,
        near_ops,
        to_target,
    )


def solution(mesh, sizes=(4, 8, 2)):
    rows = P(("morton", "grp"), None)
    placed = (
        rows,
        rows,
        P("morton", None),
        rows,
        rows,
        P(("morton", "grp")),
        rows,
        rows,
        P(),
        P(),
        P(),
    )
    return jax.shard_map(
        functools.partial(shards, sizes), mesh=mesh, in_specs=placed, out_specs=rows, check_vma=False
    )
```
